64 devices in a mesh: rep: 8 (over x, y, core), dp: 8 (over z).
Axes of the slice: x: 2, y: 2, z: 8, core: 2. Of those that a mesh axis runs over, the one named last changes fastest.
The devices are a block of a 4x4x8 slice.
Arguments:
- g_w_gate: bfloat16 [64, 2, 896, 2560], P(('rep', 'dp')), parts along dimension 0
- g_w_up: bfloat16 [64, 2, 896, 2560], P(('rep', 'dp')), parts along dimension 0
- g_w_down: bfloat16 [64, 2, 2560, 896], P(('rep', 'dp')), parts along dimension 0
- w_gate: bfloat16 [2, 896, 2560], replicated
- w_up: bfloat16 [2, 896, 2560], replicated
- w_down: bfloat16 [2, 2560, 896], replicated
- m_w_gate: float32 [2, 896, 2560], P(None, 'dp')
- m_w_up: float32 [2, 896, 2560], P(None, 'dp')
- m_w_down: float32 [2, 2560, 896], P(None, 'dp')
- v_w_gate: float32 [2, 896, 2560], P(None, 'dp')
- v_w_up: float32 [2, 896, 2560], P(None, 'dp')
- v_w_down: float32 [2, 2560, 896], P(None, 'dp')
Outputs:
- output 1: bfloat16 [16, 896, 2560], P('rep'), parts along dimension 0
- output 2: bfloat16 [16, 896, 2560], P('rep'), parts along dimension 0
- output 3: bfloat16 [16, 2560, 896], P('rep'), parts along dimension 0
- output 4: float32 [16, 896, 2560], P('rep', 'dp'), parts along dimension 0
- output 5: float32 [16, 896, 2560], P('rep', 'dp'), parts along dimension 0
- output 6: float32 [16, 2560, 896], P('rep', 'dp'), parts along dimension 0
- output 7: float32 [16, 896, 2560], P('rep', 'dp'), parts along dimension 0
- output 8: float32 [16, 896, 2560], P('rep', 'dp'), parts along dimension 0
- output 9: float32 [16, 2560, 896], P('rep', 'dp'), parts along dimension 0
There are 8 independent parts. The reference program is written for one: setup_inputs(seed, part) draws one part's arguments, and reference() takes and returns one part's arrays. A program takes and returns all parts, laid end to end along the dimension named above; an argument that names none is the same for every part.
All inputs are finite; a program needn't handle non-finite values.
Results may differ from the reference program's by a relative error of at most 0.022.
Values are sent between devices in bfloat16 or wider.
A program may use at most 768 MiB of HBM per device.

```python
import jax
import jax.numpy as jnp
from jax import lax

DEVICES = 8
D = 896
FF = 2560
LAYERS = 2
NAMES = ("w_gate", "w_up", "w_down")
SHAPES = {"w_gate": (LAYERS, D, FF), "w_up": (LAYERS, D, FF), "w_down": (LAYERS, FF, D)}


def setup_inputs(seed: int = 0, part: int = 0) -> dict:
    kz, *keys = jax.random.split(jax.random.key(seed), 1 + 5 * len(NAMES))
    loud = 2.0 ** jax.random.uniform(kz, (), jnp.float32, -1.0, 1.0)
    drawn = {}
    for name, key, both in zip(NAMES, keys[:3], keys[3:6], strict=True):
        own = jax.random.normal(jax.random.fold_in(key, part), (DEVICES, *SHAPES[name]), jnp.float32)
        shared = jax.random.normal(jax.random.fold_in(both, part), SHAPES[name], jnp.float32)
        drawn["g_" + name] = (loud * (0.7 * shared / DEVICES + 0.7 * own * DEVICES**-0.5)).astype(jnp.bfloat16)
    for name, key in zip(NAMES, keys[6:9], strict=True):
        drawn[name] = (jax.random.normal(key, SHAPES[name], jnp.float32) * SHAPES[name][1] ** -0.5).astype(jnp.bfloat16)
    for name, key in zip(NAMES, keys[9:12], strict=True):
        drawn["m_" + name] = loud * 0.5 * jax.random.normal(key, SHAPES[name], jnp.float32)
    for name, key in zip(NAMES, keys[12:15], strict=True):
        drawn["v_" + name] = loud * loud * jax.random.uniform(key, SHAPES[name], jnp.float32, 0.5, 1.5)
    return drawn


def adamw(w, m, v, g):
    m = 0.9 * m + 0.1 * g
    v = 0.95 * v + 0.05 * g * g
    step = m * lax.rsqrt(v + 1e-8) + 0.1 * w
    return (w - 0.02 * step).astype(jnp.bfloat16), m, v


def reference(g_w_gate, g_w_up, g_w_down, w_gate, w_up, w_down, m_w_gate, m_w_up, m_w_down, v_w_gate, v_w_up, v_w_down):
    def total(terms):
        return lax.scan(lambda so_far, term: (so_far + term.astype(jnp.float32), None), jnp.zeros(terms.shape[1:], jnp.float32), terms)[0]

    gradients = [total(terms).astype(jnp.bfloat16).astype(jnp.float32) for terms in (g_w_gate, g_w_up, g_w_down)]
    new = [
        adamw(w.astype(jnp.float32), m, v, g)
        for w, m, v, g in zip((w_gate, w_up, w_down), (m_w_gate, m_w_up, m_w_down), (v_w_gate, v_w_up, v_w_down), gradients, strict=True)
    ]
    return tuple(one[which] for which in range(3) for one in new)
```

```python
import functools

import jax
import jax.numpy as jnp
from jax import lax
from jax.experimental import pallas as pl
from jax.experimental.pallas import tpu as pltpu
from jax.sharding import PartitionSpec as P

MESH = pl.DeviceIdType.MESH
SLOTS = 3
F32, BF16 = jnp.float32, jnp.bfloat16


def tiles(rows, cols, wide):
    step = cols
    while step > wide and step % 256 == 0:
        step //= 2
    return 16, step


def kernel(n, *refs):
    terms, weights, old_m, old_v = (refs[i : i + 3] for i in (0, 3, 6, 9))
    whole, new_m, new_v = (refs[i : i + 3] for i in (12, 15, 18))
    slots, own, held = (refs[i : i + 3] for i in (21, 24, 27))
    sum_send, sum_recv, out_send, out_recv, own_sem, held_sem, m_sem, v_sem, free = refs[30:]
    me = lax.axis_index("dp")
    right, left = lax.rem(me + 1, n), lax.rem(me + n - 1, n)
    ahead, behind, way = (right, left), (left, right), (1, -1)
    units = [(w, d) for w in range(3) for d in range(2)]
    rows = [m.shape[1] for m in new_m]

    def index(d, hops):
        return lax.rem(me - way[d] * hops + 2 * n, n)

    def block(w, owner):
        return pl.ds(pl.multiple_of(owner * rows[w], rows[w]), rows[w])

    def load_own(w, d, hops):
        return pltpu.make_async_copy(terms[w].at[0, d, block(w, index(d, hops))], own[w].at[d], own_sem.at[w, d])

    def load_held(w, d):
        return pltpu.make_async_copy(weights[w].at[d, block(w, me)], held[w].at[d], held_sem.at[w, d])

    def load_m(w, d):
        return pltpu.make_async_copy(old_m[w].at[d], new_m[w].at[d], m_sem.at[w, d])

    def load_v(w, d):
        return pltpu.make_async_copy(old_v[w].at[d], new_v[w].at[d], v_sem.at[w, d])

    def pass_sum(w, d, step, source):
        slot = lax.rem(step, SLOTS)
        return pltpu.make_async_remote_copy(
            src_ref=source,
            dst_ref=slots[w].at[d, slot],
            send_sem=sum_send.at[w, d],
            recv_sem=sum_recv.at[w, d, slot],
            device_id={"dp": ahead[d]},
            device_id_type=MESH,
        )

    def pass_new(w, d, step):
        piece = whole[w].at[d, block(w, index(d, step))]
        return pltpu.make_async_remote_copy(
            src_ref=piece,
            dst_ref=piece,
            send_sem=out_send.at[w, d],
            recv_sem=out_recv.at[w, d, step],
            device_id={"dp": ahead[d]},
            device_id_type=MESH,
        )

    def slot_of(w, d, step):
        return slots[w].at[d, lax.rem(step, SLOTS)]

    def over(w, wide, body):
        high, across = tiles(rows[w], whole[w].shape[2], wide)

        @pl.loop(0, rows[w] // high)
        def _(i):
            for c in range(0, whole[w].shape[2], across):
                body(pl.ds(pl.multiple_of(i * high, high), high), pl.ds(c, across))

    for w, d in units:
        load_own(w, d, 2).start()
    barrier = pltpu.get_barrier_semaphore()
    for other in (left, right):
        pl.semaphore_signal(barrier, inc=1, device_id={"dp": other}, device_id_type=MESH)
    pl.semaphore_wait(barrier, 2)

    for w, d in units:
        pass_sum(w, d, 0, terms[w].at[0, d, block(w, index(d, 1))]).start()
    for w, d in units:
        load_held(w, d).start()
        load_m(w, d).start()
        load_v(w, d).start()

    @pl.loop(1, n - 1)
    def _(step):
        for w in range(3):
            for d in range(2):
                pass_sum(w, d, step - 1, slot_of(w, d, step - 1)).wait_recv()
                pass_sum(w, d, step - 1, slot_of(w, d, step - 1)).wait_send()
                load_own(w, d, 0).wait()

                @pl.when((step >= 2) & (step < n - 2))
                def _():
                    pl.semaphore_signal(free.at[w, d], inc=1, device_id={"dp": behind[d]}, device_id_type=MESH)

            for d in range(2):
                so_far = slot_of(w, d, step - 1)

                def add(r, c, so_far=so_far, d=d):
                    so_far[r, c] = (so_far[r, c].astype(F32) + own[w][d, r, c].astype(F32)).astype(BF16)

                over(w, 1280, add)
            for d in range(2):
                load_own(w, d, step + 2).start()

                @pl.when(step >= SLOTS)
                def _():
                    pl.semaphore_wait(free.at[w, d], 1)

            for d in range(2):
                pass_sum(w, d, step, slot_of(w, d, step - 1)).start()

    for w in range(3):
        for d in range(2):
            pass_sum(w, d, n - 2, slot_of(w, d, n - 2)).wait_recv()
            pass_sum(w, d, n - 2, slot_of(w, d, n - 2)).wait_send()
            load_own(w, d, 0).wait()
            load_held(w, d).wait()
            load_m(w, d).wait()
            load_v(w, d).wait()
        for d in range(2):
            so_far = slot_of(w, d, n - 2)

            def adamw(r, c, so_far=so_far, d=d):
                g = (so_far[r, c].astype(F32) + own[w][d, r, c].astype(F32)).astype(BF16).astype(F32)
                m = 0.9 * new_m[w][d, r, c] + 0.1 * g
                v = 0.95 * new_v[w][d, r, c] + 0.05 * g * g
                step = m * lax.rsqrt(v + 1e-8) + 0.1 * held[w][d, r, c].astype(F32)
                new_m[w][d, r, c] = m
                new_v[w][d, r, c] = v
                mine = pl.multiple_of(me * rows[w], 16) + r.start
                whole[w][d, pl.ds(pl.multiple_of(mine, 16), 16), c] = (held[w][d, r, c].astype(F32) - 0.02 * step).astype(BF16)

            over(w, 640, adamw)
        for d in range(2):
            pass_new(w, d, 0).start()

    @pl.loop(1, n - 1)
    def _(step):
        for w, d in units:
            pass_new(w, d, step - 1).wait_recv()
            pass_new(w, d, step - 1).wait_send()
            pass_new(w, d, step).start()

    for w, d in units:
        pass_new(w, d, n - 2).wait()


def put_out(*refs):
    half = len(refs) // 2
    arrays, results, sem = refs[:half], refs[half : 2 * half], refs[-1]
    copies = [pltpu.make_async_copy(a.at[d], r.at[d], sem.at[i, d]) for i, (a, r) in enumerate(zip(arrays, results, strict=True)) for d in range(2)]
    for one in copies:
        one.start()
    for one in copies:
        one.wait()


def solution(mesh):
    n = mesh.shape["dp"]

    def step(*arrays):
        terms, weights, m, v = (arrays[i : i + 3] for i in (0, 3, 6, 9))
        shard = [one.shape for one in m]
        anywhere, vmem = pl.BlockSpec(memory_space=pl.ANY), pl.BlockSpec(memory_space=pltpu.VMEM)
        dma = pltpu.SemaphoreType.DMA
        inputs = (pltpu.with_memory_space_constraint(x, pltpu.HBM) for x in (*terms, *weights, *m, *v))
        made = pl.pallas_call(
            functools.partial(kernel, n),
            out_shape=tuple(pltpu.VMEM(x.shape, x.dtype) for x in (*weights, *m, *v)),
            in_specs=[pl.BlockSpec(memory_space=pltpu.HBM)] * 12,
            out_specs=(vmem,) * 9,
            scratch_shapes=[
                *(pltpu.VMEM((2, SLOTS, *s[1:]), BF16) for s in shard),
                *(pltpu.VMEM(s, BF16) for s in shard),
                *(pltpu.VMEM(s, BF16) for s in shard),
                dma((3, 2)),
                dma((3, 2, SLOTS)),
                dma((3, 2)),
                dma((3, 2, n - 1)),
                dma((3, 2)),
                dma((3, 2)),
                dma((3, 2)),
                dma((3, 2)),
                pltpu.SemaphoreType.REGULAR((3, 2)),
            ],
            compiler_params=pltpu.CompilerParams(collective_id=0, has_side_effects=True, vmem_limit_bytes=20 * 2**20),
            name="step",
        )(*inputs)
        return pl.pallas_call(
            put_out,
            out_shape=tuple(jax.ShapeDtypeStruct(x.shape, x.dtype) for x in (*weights, *m, *v)),
            in_specs=[vmem] * 9,
            out_specs=(anywhere,) * 9,
            scratch_shapes=[dma((9, 2))],
            compiler_params=pltpu.CompilerParams(has_side_effects=True, vmem_limit_bytes=20 * 2**20),
            name="put_out",
        )(*(pltpu.with_memory_space_constraint(x, pltpu.VMEM) for x in made))

    all_of, cut = P(None, None, None), P(None, "dp", None)
    return jax.shard_map(
        step,
        mesh=mesh,
        in_specs=(P(("rep", "dp"), None, None, None),) * 3 + (all_of,) * 3 + (cut,) * 6,
        out_specs=(P("rep", None, None),) * 3 + (P("rep", "dp", None),) * 6,
        check_vma=False,
    )
```

```python
import functools

import jax
import jax.numpy as jnp
from jax import lax
from jax.experimental import pallas as pl
from jax.experimental.pallas import tpu as pltpu
from jax.sharding import PartitionSpec as P

MESH = pl.DeviceIdType.MESH
SLOTS = 3
COST = 100_000_000
F32, BF16 = jnp.float32, jnp.bfloat16


def tiles(rows, cols, wide):
    step = cols
    while step > wide and step % 256 == 0:
        step //= 2
    return 16, step


def kernel(n, *refs):
    terms, weights, old_m, old_v = (refs[i : i + 3] for i in (0, 3, 6, 9))
    whole, new_m, new_v = (refs[i : i + 3] for i in (12, 15, 18))
    last = refs[21:23]
    slots, own, held = (refs[i : i + 3] for i in (23, 26, 29))
    sum_send, sum_recv, out_send, out_recv, own_sem, held_sem, m_sem, v_sem, free = refs[32:]
    me = lax.axis_index("dp")
    right, left = lax.rem(me + 1, n), lax.rem(me + n - 1, n)
    ahead, behind, way = (right, left), (left, right), (1, -1)
    units = [(w, d) for w in range(3) for d in range(2)]
    rows = [m.shape[1] for m in new_m]

    def index(d, hops):
        return lax.rem(me - way[d] * hops + 2 * n, n)

    def block(w, owner):
        return pl.ds(pl.multiple_of(owner * rows[w], rows[w]), rows[w])

    def load_own(w, d, hops):
        return pltpu.make_async_copy(terms[w].at[0, d, block(w, index(d, hops))], own[w].at[d], own_sem.at[w, d])

    def load_held(w, d):
        return pltpu.make_async_copy(weights[w].at[d, block(w, me)], held[w].at[d], held_sem.at[w, d])

    def load_m(w, d):
        return pltpu.make_async_copy(old_m[w].at[d], new_m[w].at[d], m_sem.at[w, d])

    def load_v(w, d):
        return pltpu.make_async_copy(old_v[w].at[d], new_v[w].at[d], v_sem.at[w, d])

    def pass_sum(w, d, step, source):
        slot = lax.rem(step, SLOTS)
        return pltpu.make_async_remote_copy(
            src_ref=source,
            dst_ref=slots[w].at[d, slot],
            send_sem=sum_send.at[w, d],
            recv_sem=sum_recv.at[w, d, slot],
            device_id={"dp": ahead[d]},
            device_id_type=MESH,
        )

    def pass_new(w, d, step):
        piece = whole[w].at[d, block(w, index(d, step))]
        lands = last[d] if w == 2 and isinstance(step, int) and step == n - 3 else piece
        return pltpu.make_async_remote_copy(
            src_ref=piece,
            dst_ref=lands,
            send_sem=out_send.at[w, d],
            recv_sem=out_recv.at[w, d, step],
            device_id={"dp": ahead[d]},
            device_id_type=MESH,
        )

    def slot_of(w, d, step):
        return slots[w].at[d, lax.rem(step, SLOTS)]

    def over(w, wide, body):
        high, across = tiles(rows[w], whole[w].shape[2], wide)

        @pl.loop(0, rows[w] // high)
        def _(i):
            for c in range(0, whole[w].shape[2], across):
                body(pl.ds(pl.multiple_of(i * high, high), high), pl.ds(c, across))

    for w, d in units:
        load_own(w, d, 2).start()
    barrier = pltpu.get_barrier_semaphore()
    for other in (left, right):
        pl.semaphore_signal(barrier, inc=1, device_id={"dp": other}, device_id_type=MESH)
    pl.semaphore_wait(barrier, 2)

    for w, d in units:
        pass_sum(w, d, 0, terms[w].at[0, d, block(w, index(d, 1))]).start()
    for w, d in units:
        load_held(w, d).start()
        load_m(w, d).start()
        load_v(w, d).start()

    @pl.loop(1, n - 1)
    def _(step):
        for w in range(3):
            for d in range(2):
                pass_sum(w, d, step - 1, slot_of(w, d, step - 1)).wait_recv()
                pass_sum(w, d, step - 1, slot_of(w, d, step - 1)).wait_send()
                load_own(w, d, 0).wait()

                @pl.when((step >= 2) & (step < n - 2))
                def _():
                    pl.semaphore_signal(free.at[w, d], inc=1, device_id={"dp": behind[d]}, device_id_type=MESH)

            for d in range(2):
                so_far = slot_of(w, d, step - 1)

                def add(r, c, so_far=so_far, d=d):
                    so_far[r, c] = (so_far[r, c].astype(F32) + own[w][d, r, c].astype(F32)).astype(BF16)

                over(w, 1280, add)
            for d in range(2):
                load_own(w, d, step + 2).start()

                @pl.when(step >= SLOTS)
                def _():
                    pl.semaphore_wait(free.at[w, d], 1)

            for d in range(2):
                pass_sum(w, d, step, slot_of(w, d, step - 1)).start()

    for w in range(3):
        for d in range(2):
            pass_sum(w, d, n - 2, slot_of(w, d, n - 2)).wait_recv()
            pass_sum(w, d, n - 2, slot_of(w, d, n - 2)).wait_send()
            load_own(w, d, 0).wait()
            load_held(w, d).wait()
            load_m(w, d).wait()
            load_v(w, d).wait()
        for d in range(2):
            so_far = slot_of(w, d, n - 2)

            def adamw(r, c, so_far=so_far, d=d):
                g = (so_far[r, c].astype(F32) + own[w][d, r, c].astype(F32)).astype(BF16).astype(F32)
                m = 0.9 * new_m[w][d, r, c] + 0.1 * g
                v = 0.95 * new_v[w][d, r, c] + 0.05 * g * g
                step = m * lax.rsqrt(v + 1e-8) + 0.1 * held[w][d, r, c].astype(F32)
                new_m[w][d, r, c] = m
                new_v[w][d, r, c] = v
                mine = pl.multiple_of(me * rows[w], 16) + r.start
                whole[w][d, pl.ds(pl.multiple_of(mine, 16), 16), c] = (held[w][d, r, c].astype(F32) - 0.02 * step).astype(BF16)

            over(w, 640, adamw)
        for d in range(2):
            pass_new(w, d, 0).start()

    def forward(w, d, step):
        pass_new(w, d, step - 1).wait_recv()
        pass_new(w, d, step - 1).wait_send()
        pass_new(w, d, step).start()

    @pl.loop(1, n - 3)
    def _(step):
        for w, d in units:
            forward(w, d, step)

    for w, d in units:
        forward(w, d, n - 3)
    for w, d in units:
        if w < 2:
            forward(w, d, n - 2)
        else:
            pass_new(w, d, n - 3).wait()
    for w, d in units:
        if w < 2:
            pass_new(w, d, n - 2).wait()


def put_out(n, *refs):
    arrays, last, results, sem, block_sem = refs[:9], refs[9:11], refs[11:20], refs[20], refs[21]
    me = lax.axis_index("dp")
    rows = last[0].shape[0]
    copies = []
    for i, (a, r) in enumerate(zip(arrays, results, strict=True)):
        for d in range(2):
            if i == 2:
                for hops in range(n - 1):
                    owner = lax.rem(me + (n - hops if d == 0 else hops), n)
                    piece = pl.ds(pl.multiple_of(owner * rows, rows), rows)
                    source = last[d] if hops == n - 2 else a.at[d, piece]
                    copies.append(pltpu.make_async_copy(source, r.at[d, piece], block_sem.at[d, hops]))
            else:
                copies.append(pltpu.make_async_copy(a.at[d], r.at[d], sem.at[i, d]))
    for one in copies:
        one.start()
    for one in copies:
        one.wait()


def put_last(n, so_far, from_left, from_right, result, sem):
    me = lax.axis_index("dp")
    rows = from_left.shape[0]
    copies = []
    for d, one in enumerate((from_left, from_right)):
        owner = lax.rem(me + (1 if d == 0 else n - 1), n)
        copies.append(pltpu.make_async_copy(one, result.at[d, pl.ds(pl.multiple_of(owner * rows, rows), rows)], sem.at[d]))
    for one in copies:
        one.start()
    for one in copies:
        one.wait()


def solution(mesh):
    n = mesh.shape["dp"]

    def step(*arrays):
        terms, weights, m, v = (arrays[i : i + 3] for i in (0, 3, 6, 9))
        shard = [one.shape for one in m]
        hbm, vmem = pl.BlockSpec(memory_space=pltpu.HBM), pl.BlockSpec(memory_space=pltpu.VMEM)
        dma = pltpu.SemaphoreType.DMA
        inputs = (pltpu.with_memory_space_constraint(x, pltpu.HBM) for x in (*terms, *weights, *m, *v))
        made = pl.pallas_call(
            functools.partial(kernel, n),
            out_shape=(*(pltpu.VMEM(x.shape, x.dtype) for x in (*weights, *m, *v)), *(pltpu.VMEM(shard[2][1:], BF16),) * 2),
            in_specs=[hbm] * 12,
            out_specs=(vmem,) * 11,
            scratch_shapes=[
                *(pltpu.VMEM((2, SLOTS, *s[1:]), BF16) for s in shard),
                *(pltpu.VMEM(s, BF16) for s in shard),
                *(pltpu.VMEM(s, BF16) for s in shard),
                dma((3, 2)),
                dma((3, 2, SLOTS)),
                dma((3, 2)),
                dma((3, 2, n - 1)),
                dma((3, 2)),
                dma((3, 2)),
                dma((3, 2)),
                dma((3, 2)),
                pltpu.SemaphoreType.REGULAR((3, 2)),
            ],
            compiler_params=pltpu.CompilerParams(collective_id=0, has_side_effects=True, vmem_limit_bytes=20 * 2**20),
            name="step",
        )(*inputs)
        last_0, last_1 = made[9:]
        last = [lax.ppermute(one, "dp", [(i, (i + way) % n) for i in range(n)]) for one, way in ((last_0, 1), (last_1, -1))]
        out = pl.pallas_call(
            functools.partial(put_out, n),
            out_shape=tuple(jax.ShapeDtypeStruct(x.shape, x.dtype) for x in (*weights, *m, *v)),
            in_specs=[vmem] * 11,
            out_specs=(hbm,) * 9,
            scratch_shapes=[dma((9, 2)), dma((2, n - 1))],
            compiler_params=pltpu.CompilerParams(has_side_effects=True, vmem_limit_bytes=20 * 2**20),
            cost_estimate=pl.CostEstimate(flops=COST, bytes_accessed=80_000_000, transcendentals=0),
            name="put_out",
        )(*(pltpu.with_memory_space_constraint(x, pltpu.VMEM) for x in made))
        down = pl.pallas_call(
            functools.partial(put_last, n),
            out_shape=jax.ShapeDtypeStruct(weights[2].shape, BF16),
            in_specs=[hbm, vmem, vmem],
            out_specs=hbm,
            input_output_aliases={0: 0},
            scratch_shapes=[dma((2,))],
            compiler_params=pltpu.CompilerParams(has_side_effects=True, vmem_limit_bytes=20 * 2**20),
            name="put_last",
        )(pltpu.with_memory_space_constraint(out[2], pltpu.HBM), *(pltpu.with_memory_space_constraint(x, pltpu.VMEM) for x in last))
        return (*out[:2], down, *out[3:])

    all_of, cut = P(None, None, None), P(None, "dp", None)
    return jax.shard_map(
        step,
        mesh=mesh,
        in_specs=(P(("rep", "dp"), None, None, None),) * 3 + (all_of,) * 3 + (cut,) * 6,
        out_specs=(P("rep", None, None),) * 3 + (P("rep", "dp", None),) * 6,
        check_vma=False,
    )
```

```python
import functools

import jax
import jax.numpy as jnp
from jax import lax
from jax.experimental import pallas as pl
from jax.experimental.pallas import tpu as pltpu
from jax.sharding import PartitionSpec as P

MESH = pl.DeviceIdType.MESH
SLOTS = 3
COST = 100_000_000
ROOM = 17 * 2**20
F32, BF16 = jnp.float32, jnp.bfloat16


def tiles(rows, cols, wide):
    step = cols
    while step > wide and step % 256 == 0:
        step //= 2
    return 16, step


def kernel(n, *refs):
    terms, weights, old_m, old_v = (refs[i : i + 3] for i in (0, 3, 6, 9))
    whole, new_m, new_v = (refs[i : i + 3] for i in (12, 15, 18))
    last = refs[21:23]
    slots, own, held = (refs[i : i + 3] for i in (23, 26, 29))
    sum_send, sum_recv, out_send, out_recv, own_sem, held_sem, m_sem, v_sem, free = refs[32:]
    me = lax.axis_index("dp")
    right, left = lax.rem(me + 1, n), lax.rem(me + n - 1, n)
    ahead, behind, way = (right, left), (left, right), (1, -1)
    order = (2, 0, 1)
    units = [(w, d) for w in order for d in range(2)]
    rows = [m.shape[1] for m in new_m]

    def index(d, hops):
        return lax.rem(me - way[d] * hops + 2 * n, n)

    def block(w, owner):
        return pl.ds(pl.multiple_of(owner * rows[w], rows[w]), rows[w])

    def load_own(w, d, hops):
        return pltpu.make_async_copy(terms[w].at[0, d, block(w, index(d, hops))], own[w].at[d], own_sem.at[w, d])

    def load_held(w, d):
        return pltpu.make_async_copy(weights[w].at[d, block(w, me)], held[w].at[d], held_sem.at[w, d])

    def load_m(w, d):
        return pltpu.make_async_copy(old_m[w].at[d], new_m[w].at[d], m_sem.at[w, d])

    def load_v(w, d):
        return pltpu.make_async_copy(old_v[w].at[d], new_v[w].at[d], v_sem.at[w, d])

    def pass_sum(w, d, step, source):
        slot = lax.rem(step, SLOTS)
        return pltpu.make_async_remote_copy(
            src_ref=source,
            dst_ref=slots[w].at[d, slot],
            send_sem=sum_send.at[w, d],
            recv_sem=sum_recv.at[w, d, slot],
            device_id={"dp": ahead[d]},
            device_id_type=MESH,
        )

    def pass_new(w, d, step):
        piece = whole[w].at[d, block(w, index(d, step))]
        lands = last[d].at[w] if w < 2 and isinstance(step, int) and step == n - 3 else piece
        return pltpu.make_async_remote_copy(
            src_ref=piece,
            dst_ref=lands,
            send_sem=out_send.at[w, d],
            recv_sem=out_recv.at[w, d, step],
            device_id={"dp": ahead[d]},
            device_id_type=MESH,
        )

    def slot_of(w, d, step):
        return slots[w].at[d, lax.rem(step, SLOTS)]

    def over(w, wide, body):
        high, across = tiles(rows[w], whole[w].shape[2], wide)

        @pl.loop(0, rows[w] // high)
        def _(i):
            for c in range(0, whole[w].shape[2], across):
                body(pl.ds(pl.multiple_of(i * high, high), high), pl.ds(c, across))

    for w, d in units:
        load_own(w, d, 2).start()
    barrier = pltpu.get_barrier_semaphore()
    for other in (left, right):
        pl.semaphore_signal(barrier, inc=1, device_id={"dp": other}, device_id_type=MESH)
    pl.semaphore_wait(barrier, 2)

    late = lax.rem(lax.axis_index("rep"), 2) == 0
    for w, d in units:
        load_held(w, d).start()
        load_m(w, d).start()
        load_v(w, d).start()

    @pl.when(late)
    def _():
        for w, d in units:
            load_held(w, d).wait()
            load_m(w, d).wait()
            load_v(w, d).wait()

    for w, d in units:
        pass_sum(w, d, 0, terms[w].at[0, d, block(w, index(d, 1))]).start()

    @pl.loop(1, n - 1)
    def _(step):
        for w in order:
            for d in range(2):
                pass_sum(w, d, step - 1, slot_of(w, d, step - 1)).wait_recv()
                pass_sum(w, d, step - 1, slot_of(w, d, step - 1)).wait_send()
                load_own(w, d, 0).wait()

                @pl.when((step >= 2) & (step < n - 2))
                def _():
                    pl.semaphore_signal(free.at[w, d], inc=1, device_id={"dp": behind[d]}, device_id_type=MESH)

            for d in range(2):
                so_far = slot_of(w, d, step - 1)

                def add(r, c, so_far=so_far, d=d):
                    so_far[r, c] = (so_far[r, c].astype(F32) + own[w][d, r, c].astype(F32)).astype(BF16)

                over(w, 1280, add)
            for d in range(2):
                load_own(w, d, step + 2).start()

                @pl.when(step >= SLOTS)
                def _():
                    pl.semaphore_wait(free.at[w, d], 1)

            for d in range(2):
                pass_sum(w, d, step, slot_of(w, d, step - 1)).start()

    for w in order:
        for d in range(2):
            pass_sum(w, d, n - 2, slot_of(w, d, n - 2)).wait_recv()
            pass_sum(w, d, n - 2, slot_of(w, d, n - 2)).wait_send()
            load_own(w, d, 0).wait()

            @pl.when(jnp.logical_not(late))
            def _():
                load_held(w, d).wait()
                load_m(w, d).wait()
                load_v(w, d).wait()

        for d in range(2):
            so_far = slot_of(w, d, n - 2)

            def adamw(r, c, so_far=so_far, d=d):
                g = (so_far[r, c].astype(F32) + own[w][d, r, c].astype(F32)).astype(BF16).astype(F32)
                m = 0.9 * new_m[w][d, r, c] + 0.1 * g
                v = 0.95 * new_v[w][d, r, c] + 0.05 * g * g
                step = m * lax.rsqrt(v + 1e-8) + 0.1 * held[w][d, r, c].astype(F32)
                new_m[w][d, r, c] = m
                new_v[w][d, r, c] = v
                mine = pl.multiple_of(me * rows[w], 16) + r.start
                whole[w][d, pl.ds(pl.multiple_of(mine, 16), 16), c] = (held[w][d, r, c].astype(F32) - 0.02 * step).astype(BF16)

            over(w, 640, adamw)
        for d in range(2):
            pass_new(w, d, 0).start()

    def forward(w, d, step):
        pass_new(w, d, step - 1).wait_recv()
        pass_new(w, d, step - 1).wait_send()
        pass_new(w, d, step).start()

    @pl.loop(1, n - 3)
    def _(step):
        for w, d in units:
            forward(w, d, step)

    for w, d in units:
        forward(w, d, n - 3)
    for w, d in units:
        if w == 2:
            forward(w, d, n - 2)
        else:
            pass_new(w, d, n - 3).wait()
    for d in range(2):
        pass_new(2, d, n - 2).wait()


def put_out(n, *refs):
    arrays, last, results, sem, block_sem = refs[:9], refs[9:11], refs[11:20], refs[20], refs[21]
    me = lax.axis_index("dp")
    rows = last[0].shape[1]
    copies = []
    for i, (a, r) in enumerate(zip(arrays, results, strict=True)):
        for d in range(2):
            if i < 2:
                for hops in range(n - 1):
                    owner = lax.rem(me + (n - hops if d == 0 else hops), n)
                    piece = pl.ds(pl.multiple_of(owner * rows, rows), rows)
                    source = last[d].at[i] if hops == n - 2 else a.at[d, piece]
                    copies.append(pltpu.make_async_copy(source, r.at[d, piece], block_sem.at[i, d, hops]))
            else:
                copies.append(pltpu.make_async_copy(a.at[d], r.at[d], sem.at[i, d]))
    for one in copies:
        one.start()
    for one in copies:
        one.wait()


def put_last(n, gate, up, from_left, from_right, new_gate, new_up, sem):
    me = lax.axis_index("dp")
    rows = from_left.shape[1]
    copies = []
    for d, one in enumerate((from_left, from_right)):
        owner = lax.rem(me + (1 if d == 0 else n - 1), n)
        for i, result in enumerate((new_gate, new_up)):
            copies.append(pltpu.make_async_copy(one.at[i], result.at[d, pl.ds(pl.multiple_of(owner * rows, rows), rows)], sem.at[i, d]))
    for one in copies:
        one.start()
    for one in copies:
        one.wait()


def solution(mesh):
    n = mesh.shape["dp"]

    def step(*arrays):
        terms, weights, m, v = (arrays[i : i + 3] for i in (0, 3, 6, 9))
        shard = [one.shape for one in m]
        hbm, vmem = pl.BlockSpec(memory_space=pltpu.HBM), pl.BlockSpec(memory_space=pltpu.VMEM)
        dma = pltpu.SemaphoreType.DMA
        inputs = (pltpu.with_memory_space_constraint(x, pltpu.HBM) for x in (*terms, *weights, *m, *v))
        made = pl.pallas_call(
            functools.partial(kernel, n),
            out_shape=(*(pltpu.VMEM(x.shape, x.dtype) for x in (*weights, *m, *v)), *(pltpu.VMEM((2, *shard[0][1:]), BF16),) * 2),
            in_specs=[hbm] * 12,
            out_specs=(vmem,) * 11,
            scratch_shapes=[
                *(pltpu.VMEM((2, SLOTS, *s[1:]), BF16) for s in shard),
                *(pltpu.VMEM(s, BF16) for s in shard),
                *(pltpu.VMEM(s, BF16) for s in shard),
                dma((3, 2)),
                dma((3, 2, SLOTS)),
                dma((3, 2)),
                dma((3, 2, n - 1)),
                dma((3, 2)),
                dma((3, 2)),
                dma((3, 2)),
                dma((3, 2)),
                pltpu.SemaphoreType.REGULAR((3, 2)),
            ],
            compiler_params=pltpu.CompilerParams(collective_id=0, has_side_effects=True, vmem_limit_bytes=ROOM),
            name="step",
        )(*inputs)
        last_0, last_1 = made[9:]
        last = [lax.ppermute(one, "dp", [(i, (i + way) % n) for i in range(n)]) for one, way in ((last_0, 1), (last_1, -1))]
        out = pl.pallas_call(
            functools.partial(put_out, n),
            out_shape=tuple(jax.ShapeDtypeStruct(x.shape, x.dtype) for x in (*weights, *m, *v)),
            in_specs=[vmem] * 11,
            out_specs=(hbm,) * 9,
            scratch_shapes=[dma((9, 2)), dma((2, 2, n - 1))],
            compiler_params=pltpu.CompilerParams(has_side_effects=True, vmem_limit_bytes=ROOM),
            cost_estimate=pl.CostEstimate(flops=COST, bytes_accessed=80_000_000, transcendentals=0),
            name="put_out",
        )(*(pltpu.with_memory_space_constraint(x, pltpu.VMEM) for x in made))
        first = pl.pallas_call(
            functools.partial(put_last, n),
            out_shape=tuple(jax.ShapeDtypeStruct(x.shape, x.dtype) for x in weights[:2]),
            in_specs=[hbm, hbm, vmem, vmem],
            out_specs=(hbm, hbm),
            input_output_aliases={0: 0, 1: 1},
            scratch_shapes=[dma((2, 2))],
            compiler_params=pltpu.CompilerParams(has_side_effects=True, vmem_limit_bytes=ROOM),
            name="put_last",
        )(*(pltpu.with_memory_space_constraint(x, pltpu.HBM) for x in out[:2]), *(pltpu.with_memory_space_constraint(x, pltpu.VMEM) for x in last))
        return (*first, *out[2:])

    all_of, cut = P(None, None, None), P(None, "dp", None)
    return jax.shard_map(
        step,
        mesh=mesh,
        in_specs=(P(("rep", "dp"), None, None, None),) * 3 + (all_of,) * 3 + (cut,) * 6,
        out_specs=(P("rep", None, None),) * 3 + (P("rep", "dp", None),) * 6,
        check_vma=False,
    )
```

```python
import functools

import jax
import jax.numpy as jnp
from jax import lax
from jax.experimental import pallas as pl
from jax.experimental.pallas import tpu as pltpu
from jax.sharding import PartitionSpec as P

MESH = pl.DeviceIdType.MESH
SLOTS = 3
COST = 100_000_000
ROOM = 17 * 2**20
F32, BF16 = jnp.float32, jnp.bfloat16


def tiles(rows, cols, wide):
    step = cols
    while step > wide and step % 256 == 0:
        step //= 2
    return 16, step


def kernel(n, *refs):
    terms, weights, old_m, old_v = (refs[i : i + 3] for i in (0, 3, 6, 9))
    whole, new_m, new_v = (refs[i : i + 3] for i in (12, 15, 18))
    last = (refs[21:23], refs[23:25])
    slots, own, held = (refs[i : i + 3] for i in (25, 28, 31))
    sum_send, sum_recv, out_send, out_recv, own_sem, held_sem, m_sem, v_sem, free = refs[34:]
    me = lax.axis_index("dp")
    right, left = lax.rem(me + 1, n), lax.rem(me + n - 1, n)
    ahead, behind, way = (right, left), (left, right), (1, -1)
    order = (2, 0, 1)
    units = [(w, d) for w in order for d in range(2)]
    rows = [m.shape[1] for m in new_m]

    def index(d, hops):
        return lax.rem(me - way[d] * hops + 2 * n, n)

    def block(w, owner):
        return pl.ds(pl.multiple_of(owner * rows[w], rows[w]), rows[w])

    def load_own(w, d, hops):
        return pltpu.make_async_copy(terms[w].at[0, d, block(w, index(d, hops))], own[w].at[d], own_sem.at[w, d])

    def load_held(w, d):
        return pltpu.make_async_copy(weights[w].at[d, block(w, me)], held[w].at[d], held_sem.at[w, d])

    def load_m(w, d):
        return pltpu.make_async_copy(old_m[w].at[d], new_m[w].at[d], m_sem.at[w, d])

    def load_v(w, d):
        return pltpu.make_async_copy(old_v[w].at[d], new_v[w].at[d], v_sem.at[w, d])

    def pass_sum(w, d, step, source):
        slot = lax.rem(step, SLOTS)
        return pltpu.make_async_remote_copy(
            src_ref=source,
            dst_ref=slots[w].at[d, slot],
            send_sem=sum_send.at[w, d],
            recv_sem=sum_recv.at[w, d, slot],
            device_id={"dp": ahead[d]},
            device_id_type=MESH,
        )

    def pass_new(w, d, step):
        piece = whole[w].at[d, block(w, index(d, step))]
        lands = last[w][d] if w < 2 and isinstance(step, int) and step == n - 3 else piece
        return pltpu.make_async_remote_copy(
            src_ref=piece,
            dst_ref=lands,
            send_sem=out_send.at[w, d],
            recv_sem=out_recv.at[w, d, step],
            device_id={"dp": ahead[d]},
            device_id_type=MESH,
        )

    def slot_of(w, d, step):
        return slots[w].at[d, lax.rem(step, SLOTS)]

    def over(w, wide, body):
        high, across = tiles(rows[w], whole[w].shape[2], wide)

        @pl.loop(0, rows[w] // high)
        def _(i):
            for c in range(0, whole[w].shape[2], across):
                body(pl.ds(pl.multiple_of(i * high, high), high), pl.ds(c, across))

    barrier = pltpu.get_barrier_semaphore()
    for other in (left, right):
        pl.semaphore_signal(barrier, inc=1, device_id={"dp": other}, device_id_type=MESH)
    pl.semaphore_wait(barrier, 2)

    late = lax.rem(lax.axis_index("rep"), 2) == 0

    def load_rest():
        for w, d in units:
            load_own(w, d, 2).start()
            load_held(w, d).start()
            load_m(w, d).start()
            load_v(w, d).start()

    @pl.when(late)
    def _():
        load_rest()
        for w, d in units:
            load_held(w, d).wait()
            load_m(w, d).wait()
            load_v(w, d).wait()

    for w, d in units:
        pass_sum(w, d, 0, terms[w].at[0, d, block(w, index(d, 1))]).start()
    pl.when(jnp.logical_not(late))(load_rest)

    @pl.loop(1, n - 1)
    def _(step):
        for w in order:
            for d in range(2):
                pass_sum(w, d, step - 1, slot_of(w, d, step - 1)).wait_recv()
                pass_sum(w, d, step - 1, slot_of(w, d, step - 1)).wait_send()
                load_own(w, d, 0).wait()

                @pl.when((step >= 2) & (step < n - 2))
                def _():
                    pl.semaphore_signal(free.at[w, d], inc=1, device_id={"dp": behind[d]}, device_id_type=MESH)

            for d in range(2):
                so_far = slot_of(w, d, step - 1)

                def add(r, c, so_far=so_far, d=d):
                    so_far[r, c] = (so_far[r, c].astype(F32) + own[w][d, r, c].astype(F32)).astype(BF16)

                over(w, 1280, add)
            for d in range(2):
                load_own(w, d, step + 2).start()

                @pl.when(step >= SLOTS)
                def _():
                    pl.semaphore_wait(free.at[w, d], 1)

            for d in range(2):
                pass_sum(w, d, step, slot_of(w, d, step - 1)).start()

    for w in order:
        for d in range(2):
            pass_sum(w, d, n - 2, slot_of(w, d, n - 2)).wait_recv()
            pass_sum(w, d, n - 2, slot_of(w, d, n - 2)).wait_send()
            load_own(w, d, 0).wait()

            @pl.when(jnp.logical_not(late))
            def _():
                load_held(w, d).wait()
                load_m(w, d).wait()
                load_v(w, d).wait()

        for d in range(2):
            so_far = slot_of(w, d, n - 2)

            def adamw(r, c, so_far=so_far, d=d):
                g = (so_far[r, c].astype(F32) + own[w][d, r, c].astype(F32)).astype(BF16).astype(F32)
                m = 0.9 * new_m[w][d, r, c] + 0.1 * g
                v = 0.95 * new_v[w][d, r, c] + 0.05 * g * g
                step = m * lax.rsqrt(v + 1e-8) + 0.1 * held[w][d, r, c].astype(F32)
                new_m[w][d, r, c] = m
                new_v[w][d, r, c] = v
                mine = pl.multiple_of(me * rows[w], 16) + r.start
                whole[w][d, pl.ds(pl.multiple_of(mine, 16), 16), c] = (held[w][d, r, c].astype(F32) - 0.02 * step).astype(BF16)

            over(w, 640, adamw)
        for d in range(2):
            pass_new(w, d, 0).start()

    def forward(w, d, step):
        pass_new(w, d, step - 1).wait_recv()
        pass_new(w, d, step - 1).wait_send()
        pass_new(w, d, step).start()

    @pl.loop(1, n - 3)
    def _(step):
        for w, d in units:
            forward(w, d, step)

    for w, d in units:
        forward(w, d, n - 3)
    for w, d in units:
        if w == 2:
            forward(w, d, n - 2)
        else:
            pass_new(w, d, n - 3).wait()
    for d in range(2):
        pass_new(2, d, n - 2).wait()


def put_out(n, *refs):
    arrays, last, results, sem, block_sem = refs[:9], (refs[9:11], refs[11:13]), refs[13:22], refs[22], refs[23]
    me = lax.axis_index("dp")
    rows = last[0][0].shape[0]
    copies = []
    for i, (a, r) in enumerate(zip(arrays, results, strict=True)):
        for d in range(2):
            if i < 2:
                for hops in range(n - 1):
                    owner = lax.rem(me + (n - hops if d == 0 else hops), n)
                    piece = pl.ds(pl.multiple_of(owner * rows, rows), rows)
                    source = last[i][d] if hops == n - 2 else a.at[d, piece]
                    copies.append(pltpu.make_async_copy(source, r.at[d, piece], block_sem.at[i, d, hops]))
            else:
                copies.append(pltpu.make_async_copy(a.at[d], r.at[d], sem.at[i, d]))
    for one in copies:
        one.start()
    for one in copies:
        one.wait()


def put_last(n, so_far, from_left, from_right, result, sem):
    me = lax.axis_index("dp")
    rows = from_left.shape[0]
    copies = []
    for d, one in enumerate((from_left, from_right)):
        owner = lax.rem(me + (1 if d == 0 else n - 1), n)
        copies.append(pltpu.make_async_copy(one, result.at[d, pl.ds(pl.multiple_of(owner * rows, rows), rows)], sem.at[d]))
    for one in copies:
        one.start()
    for one in copies:
        one.wait()


def solution(mesh):
    n = mesh.shape["dp"]

    def step(*arrays):
        terms, weights, m, v = (arrays[i : i + 3] for i in (0, 3, 6, 9))
        shard = [one.shape for one in m]
        hbm, vmem = pl.BlockSpec(memory_space=pltpu.HBM), pl.BlockSpec(memory_space=pltpu.VMEM)
        dma = pltpu.SemaphoreType.DMA
        inputs = (pltpu.with_memory_space_constraint(x, pltpu.HBM) for x in (*terms, *weights, *m, *v))
        made = pl.pallas_call(
            functools.partial(kernel, n),
            out_shape=(*(pltpu.VMEM(x.shape, x.dtype) for x in (*weights, *m, *v)), *(pltpu.VMEM(shard[0][1:], BF16),) * 4),
            in_specs=[hbm] * 12,
            out_specs=(vmem,) * 13,
            scratch_shapes=[
                *(pltpu.VMEM((2, SLOTS, *s[1:]), BF16) for s in shard),
                *(pltpu.VMEM(s, BF16) for s in shard),
                *(pltpu.VMEM(s, BF16) for s in shard),
                dma((3, 2)),
                dma((3, 2, SLOTS)),
                dma((3, 2)),
                dma((3, 2, n - 1)),
                dma((3, 2)),
                dma((3, 2)),
                dma((3, 2)),
                dma((3, 2)),
                pltpu.SemaphoreType.REGULAR((3, 2)),
            ],
            compiler_params=pltpu.CompilerParams(collective_id=0, has_side_effects=True, vmem_limit_bytes=ROOM),
            name="step",
        )(*inputs)
        rings = [[(i, (i + way) % n) for i in range(n)] for way in (1, -1)]
        last = [[lax.ppermute(made[9 + 2 * w + d], "dp", rings[d]) for d in range(2)] for w in range(2)]
        out = pl.pallas_call(
            functools.partial(put_out, n),
            out_shape=tuple(jax.ShapeDtypeStruct(x.shape, x.dtype) for x in (*weights, *m, *v)),
            in_specs=[vmem] * 13,
            out_specs=(hbm,) * 9,
            scratch_shapes=[dma((9, 2)), dma((2, 2, n - 1))],
            compiler_params=pltpu.CompilerParams(has_side_effects=True, vmem_limit_bytes=ROOM),
            cost_estimate=pl.CostEstimate(flops=COST, bytes_accessed=80_000_000, transcendentals=0),
            name="put_out",
        )(*(pltpu.with_memory_space_constraint(x, pltpu.VMEM) for x in made))
        first = [
            pl.pallas_call(
                functools.partial(put_last, n),
                out_shape=jax.ShapeDtypeStruct(weights[w].shape, BF16),
                in_specs=[hbm, vmem, vmem],
                out_specs=hbm,
                input_output_aliases={0: 0},
                scratch_shapes=[dma((2,))],
                compiler_params=pltpu.CompilerParams(has_side_effects=True, vmem_limit_bytes=ROOM),
                name="put_last",
            )(pltpu.with_memory_space_constraint(out[w], pltpu.HBM), *(pltpu.with_memory_space_constraint(x, pltpu.VMEM) for x in last[w]))
            for w in range(2)
        ]
        return (*first, *out[2:])

    all_of, cut = P(None, None, None), P(None, "dp", None)
    return jax.shard_map(
        step,
        mesh=mesh,
        in_specs=(P(("rep", "dp"), None, None, None),) * 3 + (all_of,) * 3 + (cut,) * 6,
        out_specs=(P("rep", None, None),) * 3 + (P("rep", "dp", None),) * 6,
        check_vma=False,
    )
```

```python
import functools

import jax
import jax.numpy as jnp
from jax import lax
from jax.experimental import pallas as pl
from jax.experimental.pallas import tpu as pltpu
from jax.sharding import PartitionSpec as P

MESH = pl.DeviceIdType.MESH
SLOTS = 3
TAIL = 32
COST = 100_000_000
ROOM = 17 * 2**20
F32, BF16 = jnp.float32, jnp.bfloat16


def tiles(rows, cols, wide):
    step = cols
    while step > wide and step % 256 == 0:
        step //= 2
    return 16, step


def kernel(n, *refs):
    terms, weights, old_m, old_v = (refs[i : i + 3] for i in (0, 3, 6, 9))
    whole, new_m, new_v = (refs[i : i + 3] for i in (12, 15, 18))
    most, rest = refs[21:23], refs[23:25]
    slots, own, held = (refs[i : i + 3] for i in (25, 28, 31))
    sum_send, sum_recv, out_send, out_recv, own_sem, held_sem, m_sem, v_sem, rest_send, rest_recv, free = refs[34:]
    me = lax.axis_index("dp")
    right, left = lax.rem(me + 1, n), lax.rem(me + n - 1, n)
    ahead, behind, way = (right, left), (left, right), (1, -1)
    order = (2, 0, 1)
    units = [(w, d) for w in order for d in range(2)]
    rows = [m.shape[1] for m in new_m]

    def index(d, hops):
        return lax.rem(me - way[d] * hops + 2 * n, n)

    def block(w, owner):
        return pl.ds(pl.multiple_of(owner * rows[w], rows[w]), rows[w])

    def load_own(w, d, hops):
        return pltpu.make_async_copy(terms[w].at[0, d, block(w, index(d, hops))], own[w].at[d], own_sem.at[w, d])

    def load_held(w, d):
        return pltpu.make_async_copy(weights[w].at[d, block(w, me)], held[w].at[d], held_sem.at[w, d])

    def load_m(w, d):
        return pltpu.make_async_copy(old_m[w].at[d], new_m[w].at[d], m_sem.at[w, d])

    def load_v(w, d):
        return pltpu.make_async_copy(old_v[w].at[d], new_v[w].at[d], v_sem.at[w, d])

    def pass_sum(w, d, step, source):
        slot = lax.rem(step, SLOTS)
        return pltpu.make_async_remote_copy(
            src_ref=source,
            dst_ref=slots[w].at[d, slot],
            send_sem=sum_send.at[w, d],
            recv_sem=sum_recv.at[w, d, slot],
            device_id={"dp": ahead[d]},
            device_id_type=MESH,
        )

    def pass_new(w, d, step):
        piece = whole[w].at[d, block(w, index(d, step))]
        lands = piece
        if isinstance(step, int) and step == n - 3 and w < 2:
            first, count = (0, rows[0]) if w == 0 else (rows[0], rows[1] - TAIL)
            piece = whole[w].at[d, pl.ds(pl.multiple_of(index(d, step) * rows[w], rows[w]), count)]
            lands = most[d].at[pl.ds(first, count)]
        return pltpu.make_async_remote_copy(
            src_ref=piece,
            dst_ref=lands,
            send_sem=out_send.at[w, d],
            recv_sem=out_recv.at[w, d, step],
            device_id={"dp": ahead[d]},
            device_id_type=MESH,
        )

    def pass_rest(d):
        first = pl.multiple_of(index(d, n - 3) * rows[1] + (rows[1] - TAIL), 16)
        return pltpu.make_async_remote_copy(
            src_ref=whole[1].at[d, pl.ds(first, TAIL)],
            dst_ref=rest[d],
            send_sem=rest_send.at[d],
            recv_sem=rest_recv.at[d],
            device_id={"dp": ahead[d]},
            device_id_type=MESH,
        )

    def slot_of(w, d, step):
        return slots[w].at[d, lax.rem(step, SLOTS)]

    def over(w, wide, body):
        high, across = tiles(rows[w], whole[w].shape[2], wide)

        @pl.loop(0, rows[w] // high)
        def _(i):
            for c in range(0, whole[w].shape[2], across):
                body(pl.ds(pl.multiple_of(i * high, high), high), pl.ds(c, across))

    barrier = pltpu.get_barrier_semaphore()
    for other in (left, right):
        pl.semaphore_signal(barrier, inc=1, device_id={"dp": other}, device_id_type=MESH)
    pl.semaphore_wait(barrier, 2)

    late = lax.rem(lax.axis_index("rep"), 2) == 0

    def load_rest():
        for w, d in units:
            load_held(w, d).start()
            load_m(w, d).start()
        for w, d in units:
            load_own(w, d, 2).start()
            load_v(w, d).start()

    @pl.when(late)
    def _():
        load_rest()
        for w, d in units:
            load_held(w, d).wait()
            load_m(w, d).wait()

    for w, d in units:
        pass_sum(w, d, 0, terms[w].at[0, d, block(w, index(d, 1))]).start()
    pl.when(jnp.logical_not(late))(load_rest)

    @pl.loop(1, n - 1)
    def _(step):
        for w in order:
            for d in range(2):
                pass_sum(w, d, step - 1, slot_of(w, d, step - 1)).wait_recv()
                pass_sum(w, d, step - 1, slot_of(w, d, step - 1)).wait_send()
                load_own(w, d, 0).wait()

                @pl.when((step >= 2) & (step < n - 2))
                def _():
                    pl.semaphore_signal(free.at[w, d], inc=1, device_id={"dp": behind[d]}, device_id_type=MESH)

            for d in range(2):
                so_far = slot_of(w, d, step - 1)

                def add(r, c, so_far=so_far, d=d):
                    so_far[r, c] = (so_far[r, c].astype(F32) + own[w][d, r, c].astype(F32)).astype(BF16)

                over(w, 1280, add)
            for d in range(2):
                load_own(w, d, step + 2).start()

                @pl.when(step >= SLOTS)
                def _():
                    pl.semaphore_wait(free.at[w, d], 1)

            for d in range(2):
                pass_sum(w, d, step, slot_of(w, d, step - 1)).start()

    for w in order:
        for d in range(2):
            pass_sum(w, d, n - 2, slot_of(w, d, n - 2)).wait_recv()
            pass_sum(w, d, n - 2, slot_of(w, d, n - 2)).wait_send()
            load_own(w, d, 0).wait()

            load_v(w, d).wait()

            @pl.when(jnp.logical_not(late))
            def _():
                load_held(w, d).wait()
                load_m(w, d).wait()

        for d in range(2):
            so_far = slot_of(w, d, n - 2)

            def adamw(r, c, so_far=so_far, d=d):
                g = (so_far[r, c].astype(F32) + own[w][d, r, c].astype(F32)).astype(BF16).astype(F32)
                m = 0.9 * new_m[w][d, r, c] + 0.1 * g
                v = 0.95 * new_v[w][d, r, c] + 0.05 * g * g
                step = m * lax.rsqrt(v + 1e-8) + 0.1 * held[w][d, r, c].astype(F32)
                new_m[w][d, r, c] = m
                new_v[w][d, r, c] = v
                mine = pl.multiple_of(me * rows[w], 16) + r.start
                whole[w][d, pl.ds(pl.multiple_of(mine, 16), 16), c] = (held[w][d, r, c].astype(F32) - 0.02 * step).astype(BF16)

            over(w, 640, adamw)
        for d in range(2):
            pass_new(w, d, 0).start()

    def forward(w, d, step):
        pass_new(w, d, step - 1).wait_recv()
        pass_new(w, d, step - 1).wait_send()
        pass_new(w, d, step).start()

    @pl.loop(1, n - 3)
    def _(step):
        for w, d in units:
            forward(w, d, step)

    for w, d in units:
        forward(w, d, n - 3)
        if w == 1:
            pass_rest(d).start()
    for w, d in units:
        if w == 2:
            forward(w, d, n - 2)
        else:
            pass_new(w, d, n - 3).wait()
    for d in range(2):
        pass_rest(d).wait()
        pass_new(2, d, n - 2).wait()


def put_out(n, *refs):
    arrays, most, rest, results = refs[:9], refs[9:11], refs[11:13], refs[13:22]
    sem, block_sem, rest_sem = refs[22:]
    me = lax.axis_index("dp")
    rows = arrays[0].shape[1] // n
    copies = []
    for i, (a, r) in enumerate(zip(arrays, results, strict=True)):
        for d in range(2):
            if i < 2:
                for hops in range(n - 1):
                    owner = lax.rem(me + (n - hops if d == 0 else hops), n)
                    piece = pl.ds(pl.multiple_of(owner * rows, rows), rows)
                    source = a.at[d, piece]
                    if hops == n - 2 and i == 0:
                        source = most[d].at[pl.ds(0, rows)]
                    elif hops == n - 2:
                        piece = pl.ds(pl.multiple_of(owner * rows, rows), rows - TAIL)
                        source = most[d].at[pl.ds(rows, rows - TAIL)]
                        tail = pl.ds(pl.multiple_of(owner * rows + (rows - TAIL), 16), TAIL)
                        copies.append(pltpu.make_async_copy(rest[d], r.at[d, tail], rest_sem.at[d]))
                    copies.append(pltpu.make_async_copy(source, r.at[d, piece], block_sem.at[i, d, hops]))
            else:
                copies.append(pltpu.make_async_copy(a.at[d], r.at[d], sem.at[i, d]))
    run(copies)


def run(copies):
    for one in copies:
        one.start()
    for one in copies:
        one.wait()


def put_most(n, gate, up, from_left, from_right, new_gate, new_up, sem):
    me = lax.axis_index("dp")
    rows = gate.shape[1] // n
    copies = []
    for d, one in enumerate((from_left, from_right)):
        owner = lax.rem(me + (1 if d == 0 else n - 1), n)
        for i, (result, first, count) in enumerate(((new_gate, 0, rows), (new_up, rows, rows - TAIL))):
            piece = pl.ds(pl.multiple_of(owner * rows, rows), count)
            copies.append(pltpu.make_async_copy(one.at[pl.ds(first, count)], result.at[d, piece], sem.at[i, d]))
    run(copies)


def put_rest(n, up, from_left, from_right, new_up, sem):
    me = lax.axis_index("dp")
    rows = up.shape[1] // n
    copies = []
    for d, one in enumerate((from_left, from_right)):
        owner = lax.rem(me + (1 if d == 0 else n - 1), n)
        piece = pl.ds(pl.multiple_of(owner * rows + (rows - TAIL), 16), TAIL)
        copies.append(pltpu.make_async_copy(one, new_up.at[d, piece], sem.at[d]))
    run(copies)


def solution(mesh):
    n = mesh.shape["dp"]

    def step(*arrays):
        terms, weights, m, v = (arrays[i : i + 3] for i in (0, 3, 6, 9))
        shard = [one.shape for one in m]
        cols = shard[0][2]
        hbm, vmem = pl.BlockSpec(memory_space=pltpu.HBM), pl.BlockSpec(memory_space=pltpu.VMEM)
        dma = pltpu.SemaphoreType.DMA
        inputs = (pltpu.with_memory_space_constraint(x, pltpu.HBM) for x in (*terms, *weights, *m, *v))
        made = pl.pallas_call(
            functools.partial(kernel, n),
            out_shape=(*(pltpu.VMEM(x.shape, x.dtype) for x in (*weights, *m, *v)), *(pltpu.VMEM((rows, cols), BF16) for rows in (2 * shard[0][1] - TAIL, TAIL) for _ in range(2))),
            in_specs=[hbm] * 12,
            out_specs=(vmem,) * 13,
            scratch_shapes=[
                *(pltpu.VMEM((2, SLOTS, *s[1:]), BF16) for s in shard),
                *(pltpu.VMEM(s, BF16) for s in shard),
                *(pltpu.VMEM(s, BF16) for s in shard),
                dma((3, 2)),
                dma((3, 2, SLOTS)),
                dma((3, 2)),
                dma((3, 2, n - 1)),
                dma((3, 2)),
                dma((3, 2)),
                dma((3, 2)),
                dma((3, 2)),
                dma((2,)),
                dma((2,)),
                pltpu.SemaphoreType.REGULAR((3, 2)),
            ],
            compiler_params=pltpu.CompilerParams(collective_id=0, has_side_effects=True, vmem_limit_bytes=ROOM),
            name="step",
        )(*inputs)
        rings = [[(i, (i + way) % n) for i in range(n)] for way in (1, -1)]
        most, rest = ([lax.ppermute(made[at + d], "dp", rings[d]) for d in range(2)] for at in (9, 11))
        out = pl.pallas_call(
            functools.partial(put_out, n),
            out_shape=tuple(jax.ShapeDtypeStruct(x.shape, x.dtype) for x in (*weights, *m, *v)),
            in_specs=[vmem] * 13,
            out_specs=(hbm,) * 9,
            scratch_shapes=[dma((9, 2)), dma((2, 2, n - 1)), dma((2,))],
            compiler_params=pltpu.CompilerParams(has_side_effects=True, vmem_limit_bytes=ROOM),
            cost_estimate=pl.CostEstimate(flops=COST, bytes_accessed=80_000_000, transcendentals=0),
            name="put_out",
        )(*(pltpu.with_memory_space_constraint(x, pltpu.VMEM) for x in made))
        in_hbm, in_vmem = (functools.partial(pltpu.with_memory_space_constraint, memory_space=x) for x in (pltpu.HBM, pltpu.VMEM))
        gate, up = pl.pallas_call(
            functools.partial(put_most, n),
            out_shape=tuple(jax.ShapeDtypeStruct(x.shape, BF16) for x in weights[:2]),
            in_specs=[hbm, hbm, vmem, vmem],
            out_specs=(hbm, hbm),
            input_output_aliases={0: 0, 1: 1},
            scratch_shapes=[dma((2, 2))],
            compiler_params=pltpu.CompilerParams(has_side_effects=True, vmem_limit_bytes=ROOM),
            name="put_most",
        )(*map(in_hbm, out[:2]), *map(in_vmem, most))
        up = pl.pallas_call(
            functools.partial(put_rest, n),
            out_shape=jax.ShapeDtypeStruct(weights[1].shape, BF16),
            in_specs=[hbm, vmem, vmem],
            out_specs=hbm,
            input_output_aliases={0: 0},
            scratch_shapes=[dma((2,))],
            compiler_params=pltpu.CompilerParams(has_side_effects=True, vmem_limit_bytes=ROOM),
            name="put_rest",
        )(in_hbm(up), *map(in_vmem, rest))
        return (gate, up, *out[2:])

    all_of, cut = P(None, None, None), P(None, "dp", None)
    return jax.shard_map(
        step,
        mesh=mesh,
        in_specs=(P(("rep", "dp"), None, None, None),) * 3 + (all_of,) * 3 + (cut,) * 6,
        out_specs=(P("rep", None, None),) * 3 + (P("rep", "dp", None),) * 6,
        check_vma=False,
    )
```

```python
import functools

import jax
import jax.numpy as jnp
from jax import lax
from jax.experimental import pallas as pl
from jax.experimental.pallas import tpu as pltpu
from jax.sharding import PartitionSpec as P

MESH = pl.DeviceIdType.MESH
SLOTS = 3
TAIL = 32
COST = 100_000_000
ROOM = 17 * 2**20
F32, BF16 = jnp.float32, jnp.bfloat16


def tiles(rows, cols, wide):
    step = cols
    while step > wide and step % 256 == 0:
        step //= 2
    return 16, step


def kernel(n, *refs):
    terms, weights, old_m, old_v = (refs[i : i + 3] for i in (0, 3, 6, 9))
    whole, new_m, new_v = (refs[i : i + 3] for i in (12, 15, 18))
    most, rest = refs[21:23], refs[23:25]
    slots, own, held = (refs[i : i + 3] for i in (25, 28, 31))
    sum_send, sum_recv, out_send, out_recv, own_sem, held_sem, m_sem, v_sem, rest_send, rest_recv, here, free = refs[34:]
    me = lax.axis_index("dp")
    right, left = lax.rem(me + 1, n), lax.rem(me + n - 1, n)
    ahead, behind, way = (right, left), (left, right), (1, -1)
    order = (2, 0, 1)
    units = [(w, d) for w in order for d in range(2)]
    rows = [m.shape[1] for m in new_m]

    def index(d, hops):
        return lax.rem(me - way[d] * hops + 2 * n, n)

    def block(w, owner):
        return pl.ds(pl.multiple_of(owner * rows[w], rows[w]), rows[w])

    def load_own(w, d, hops):
        return pltpu.make_async_copy(terms[w].at[0, d, block(w, index(d, hops))], own[w].at[d], own_sem.at[w, d])

    def load_held(w, d):
        return pltpu.make_async_copy(weights[w].at[d, block(w, me)], held[w].at[d], held_sem.at[w, d])

    def load_m(w, d):
        return pltpu.make_async_copy(old_m[w].at[d], new_m[w].at[d], m_sem.at[w, d])

    def load_v(w, d):
        return pltpu.make_async_copy(old_v[w].at[d], new_v[w].at[d], v_sem.at[w, d])

    def pass_sum(w, d, step, source):
        slot = lax.rem(step, SLOTS)
        return pltpu.make_async_remote_copy(
            src_ref=source,
            dst_ref=slots[w].at[d, slot],
            send_sem=sum_send.at[w, d],
            recv_sem=sum_recv.at[w, d, slot],
            device_id={"dp": ahead[d]},
            device_id_type=MESH,
        )

    def pass_new(w, d, step):
        piece = whole[w].at[d, block(w, index(d, step))]
        lands = piece
        if isinstance(step, int) and step == n - 3 and w < 2:
            first, count = (0, rows[0]) if w == 0 else (rows[0], rows[1] - TAIL)
            piece = whole[w].at[d, pl.ds(pl.multiple_of(index(d, step) * rows[w], rows[w]), count)]
            lands = most[d].at[pl.ds(first, count)]
        return pltpu.make_async_remote_copy(
            src_ref=piece,
            dst_ref=lands,
            send_sem=out_send.at[w, d],
            recv_sem=out_recv.at[w, d, step],
            device_id={"dp": ahead[d]},
            device_id_type=MESH,
        )

    def pass_rest(d):
        first = pl.multiple_of(index(d, n - 3) * rows[1] + (rows[1] - TAIL), 16)
        return pltpu.make_async_remote_copy(
            src_ref=whole[1].at[d, pl.ds(first, TAIL)],
            dst_ref=rest[d],
            send_sem=rest_send.at[d],
            recv_sem=rest_recv.at[d],
            device_id={"dp": ahead[d]},
            device_id_type=MESH,
        )

    def slot_of(w, d, step):
        return slots[w].at[d, lax.rem(step, SLOTS)]

    def over(w, wide, body):
        high, across = tiles(rows[w], whole[w].shape[2], wide)

        @pl.loop(0, rows[w] // high)
        def _(i):
            for c in range(0, whole[w].shape[2], across):
                body(pl.ds(pl.multiple_of(i * high, high), high), pl.ds(c, across))

    barrier = pltpu.get_barrier_semaphore()
    pl.semaphore_signal(barrier, inc=1, device_id={"dp": left}, device_id_type=MESH)
    pl.semaphore_wait(barrier, 1)
    pl.semaphore_signal(here, inc=1, device_id={"dp": right}, device_id_type=MESH)

    late = lax.rem(lax.axis_index("rep"), 2) == 0

    def load_rest():
        for w, d in units:
            load_held(w, d).start()
            load_m(w, d).start()
        for w, d in units:
            load_own(w, d, 2).start()
            load_v(w, d).start()

    @pl.when(late)
    def _():
        load_rest()
        for w, d in units:
            load_held(w, d).wait()
            load_m(w, d).wait()

    def send_first(d):
        for w in order:
            pass_sum(w, d, 0, terms[w].at[0, d, block(w, index(d, 1))]).start()

    send_first(0)
    pl.when(jnp.logical_not(late))(load_rest)
    pl.semaphore_wait(here, 1)
    send_first(1)

    @pl.loop(1, n - 1)
    def _(step):
        for w in order:
            for d in range(2):
                pass_sum(w, d, step - 1, slot_of(w, d, step - 1)).wait_recv()
                pass_sum(w, d, step - 1, slot_of(w, d, step - 1)).wait_send()
                load_own(w, d, 0).wait()

                @pl.when((step >= 2) & (step < n - 2))
                def _():
                    pl.semaphore_signal(free.at[w, d], inc=1, device_id={"dp": behind[d]}, device_id_type=MESH)

            for d in range(2):
                so_far = slot_of(w, d, step - 1)

                def add(r, c, so_far=so_far, d=d):
                    so_far[r, c] = (so_far[r, c].astype(F32) + own[w][d, r, c].astype(F32)).astype(BF16)

                over(w, 1280, add)
            for d in range(2):
                load_own(w, d, step + 2).start()

                @pl.when(step >= SLOTS)
                def _():
                    pl.semaphore_wait(free.at[w, d], 1)

            for d in range(2):
                pass_sum(w, d, step, slot_of(w, d, step - 1)).start()

    for w in order:
        for d in range(2):
            pass_sum(w, d, n - 2, slot_of(w, d, n - 2)).wait_recv()
            pass_sum(w, d, n - 2, slot_of(w, d, n - 2)).wait_send()
            load_own(w, d, 0).wait()

            load_v(w, d).wait()

            @pl.when(jnp.logical_not(late))
            def _():
                load_held(w, d).wait()
                load_m(w, d).wait()

        for d in range(2):
            so_far = slot_of(w, d, n - 2)

            def adamw(r, c, so_far=so_far, d=d):
                g = (so_far[r, c].astype(F32) + own[w][d, r, c].astype(F32)).astype(BF16).astype(F32)
                m = 0.9 * new_m[w][d, r, c] + 0.1 * g
                v = 0.95 * new_v[w][d, r, c] + 0.05 * g * g
                step = m * lax.rsqrt(v + 1e-8) + 0.1 * held[w][d, r, c].astype(F32)
                new_m[w][d, r, c] = m
                new_v[w][d, r, c] = v
                mine = pl.multiple_of(me * rows[w], 16) + r.start
                whole[w][d, pl.ds(pl.multiple_of(mine, 16), 16), c] = (held[w][d, r, c].astype(F32) - 0.02 * step).astype(BF16)

            over(w, 640, adamw)
        for d in range(2):
            pass_new(w, d, 0).start()

    def forward(w, d, step):
        pass_new(w, d, step - 1).wait_recv()
        pass_new(w, d, step - 1).wait_send()
        pass_new(w, d, step).start()

    @pl.loop(1, n - 3)
    def _(step):
        for w, d in units:
            forward(w, d, step)

    for w, d in units:
        forward(w, d, n - 3)
        if w == 1:
            pass_rest(d).start()
    for w, d in units:
        if w == 2:
            forward(w, d, n - 2)
        else:
            pass_new(w, d, n - 3).wait()
    for d in range(2):
        pass_rest(d).wait()
        pass_new(2, d, n - 2).wait()


def put_out(n, *refs):
    arrays, most, rest, results = refs[:9], refs[9:11], refs[11:13], refs[13:22]
    sem, block_sem, rest_sem = refs[22:]
    me = lax.axis_index("dp")
    rows = arrays[0].shape[1] // n
    copies = []
    for i, (a, r) in enumerate(zip(arrays, results, strict=True)):
        for d in range(2):
            if i < 2:
                for hops in range(n - 1):
                    owner = lax.rem(me + (n - hops if d == 0 else hops), n)
                    piece = pl.ds(pl.multiple_of(owner * rows, rows), rows)
                    source = a.at[d, piece]
                    if hops == n - 2 and i == 0:
                        source = most[d].at[pl.ds(0, rows)]
                    elif hops == n - 2:
                        piece = pl.ds(pl.multiple_of(owner * rows, rows), rows - TAIL)
                        source = most[d].at[pl.ds(rows, rows - TAIL)]
                        tail = pl.ds(pl.multiple_of(owner * rows + (rows - TAIL), 16), TAIL)
                        copies.append(pltpu.make_async_copy(rest[d], r.at[d, tail], rest_sem.at[d]))
                    copies.append(pltpu.make_async_copy(source, r.at[d, piece], block_sem.at[i, d, hops]))
            else:
                copies.append(pltpu.make_async_copy(a.at[d], r.at[d], sem.at[i, d]))
    run(copies)


def run(copies):
    for one in copies:
        one.start()
    for one in copies:
        one.wait()


def put_most(n, gate, up, from_left, from_right, new_gate, new_up, sem):
    me = lax.axis_index("dp")
    rows = gate.shape[1] // n
    copies = []
    for d, one in enumerate((from_left, from_right)):
        owner = lax.rem(me + (1 if d == 0 else n - 1), n)
        for i, (result, first, count) in enumerate(((new_gate, 0, rows), (new_up, rows, rows - TAIL))):
            piece = pl.ds(pl.multiple_of(owner * rows, rows), count)
            copies.append(pltpu.make_async_copy(one.at[pl.ds(first, count)], result.at[d, piece], sem.at[i, d]))
    run(copies)


def put_rest(n, up, from_left, from_right, new_up, sem):
    me = lax.axis_index("dp")
    rows = up.shape[1] // n
    copies = []
    for d, one in enumerate((from_left, from_right)):
        owner = lax.rem(me + (1 if d == 0 else n - 1), n)
        piece = pl.ds(pl.multiple_of(owner * rows + (rows - TAIL), 16), TAIL)
        copies.append(pltpu.make_async_copy(one, new_up.at[d, piece], sem.at[d]))
    run(copies)


def solution(mesh):
    n = mesh.shape["dp"]

    def step(*arrays):
        terms, weights, m, v = (arrays[i : i + 3] for i in (0, 3, 6, 9))
        shard = [one.shape for one in m]
        cols = shard[0][2]
        hbm, vmem = pl.BlockSpec(memory_space=pltpu.HBM), pl.BlockSpec(memory_space=pltpu.VMEM)
        dma = pltpu.SemaphoreType.DMA
        inputs = (pltpu.with_memory_space_constraint(x, pltpu.HBM) for x in (*terms, *weights, *m, *v))
        made = pl.pallas_call(
            functools.partial(kernel, n),
            out_shape=(*(pltpu.VMEM(x.shape, x.dtype) for x in (*weights, *m, *v)), *(pltpu.VMEM((rows, cols), BF16) for rows in (2 * shard[0][1] - TAIL, TAIL) for _ in range(2))),
            in_specs=[hbm] * 12,
            out_specs=(vmem,) * 13,
            scratch_shapes=[
                *(pltpu.VMEM((2, SLOTS, *s[1:]), BF16) for s in shard),
                *(pltpu.VMEM(s, BF16) for s in shard),
                *(pltpu.VMEM(s, BF16) for s in shard),
                dma((3, 2)),
                dma((3, 2, SLOTS)),
                dma((3, 2)),
                dma((3, 2, n - 1)),
                dma((3, 2)),
                dma((3, 2)),
                dma((3, 2)),
                dma((3, 2)),
                dma((2,)),
                dma((2,)),
                pltpu.SemaphoreType.REGULAR,
                pltpu.SemaphoreType.REGULAR((3, 2)),
            ],
            compiler_params=pltpu.CompilerParams(collective_id=0, has_side_effects=True, vmem_limit_bytes=ROOM),
            name="step",
        )(*inputs)
        rings = [[(i, (i + way) % n) for i in range(n)] for way in (1, -1)]
        most, rest = ([lax.ppermute(made[at + d], "dp", rings[d]) for d in range(2)] for at in (9, 11))
        out = pl.pallas_call(
            functools.partial(put_out, n),
            out_shape=tuple(jax.ShapeDtypeStruct(x.shape, x.dtype) for x in (*weights, *m, *v)),
            in_specs=[vmem] * 13,
            out_specs=(hbm,) * 9,
            scratch_shapes=[dma((9, 2)), dma((2, 2, n - 1)), dma((2,))],
            compiler_params=pltpu.CompilerParams(has_side_effects=True, vmem_limit_bytes=ROOM),
            cost_estimate=pl.CostEstimate(flops=COST, bytes_accessed=80_000_000, transcendentals=0),
            name="put_out",
        )(*(pltpu.with_memory_space_constraint(x, pltpu.VMEM) for x in made))
        in_hbm, in_vmem = (functools.partial(pltpu.with_memory_space_constraint, memory_space=x) for x in (pltpu.HBM, pltpu.VMEM))
        gate, up = pl.pallas_call(
            functools.partial(put_most, n),
            out_shape=tuple(jax.ShapeDtypeStruct(x.shape, BF16) for x in weights[:2]),
            in_specs=[hbm, hbm, vmem, vmem],
            out_specs=(hbm, hbm),
            input_output_aliases={0: 0, 1: 1},
            scratch_shapes=[dma((2, 2))],
            compiler_params=pltpu.CompilerParams(has_side_effects=True, vmem_limit_bytes=ROOM),
            name="put_most",
        )(*map(in_hbm, out[:2]), *map(in_vmem, most))
        up = pl.pallas_call(
            functools.partial(put_rest, n),
            out_shape=jax.ShapeDtypeStruct(weights[1].shape, BF16),
            in_specs=[hbm, vmem, vmem],
            out_specs=hbm,
            input_output_aliases={0: 0},
            scratch_shapes=[dma((2,))],
            compiler_params=pltpu.CompilerParams(has_side_effects=True, vmem_limit_bytes=ROOM),
            name="put_rest",
        )(in_hbm(up), *map(in_vmem, rest))
        return (gate, up, *out[2:])

    all_of, cut = P(None, None, None), P(None, "dp", None)
    return jax.shard_map(
        step,
        mesh=mesh,
        in_specs=(P(("rep", "dp"), None, None, None),) * 3 + (all_of,) * 3 + (cut,) * 6,
        out_specs=(P("rep", None, None),) * 3 + (P("rep", "dp", None),) * 6,
        check_vma=False,
    )
```

```python
import functools

import jax
import jax.numpy as jnp
from jax import lax
from jax.experimental import pallas as pl
from jax.experimental.pallas import tpu as pltpu
from jax.sharding import PartitionSpec as P

MESH = pl.DeviceIdType.MESH
SLOTS = 3
TAIL = 32
COST = 100_000_000
ROOM = 17 * 2**20
F32, BF16 = jnp.float32, jnp.bfloat16


def tiles(rows, cols, wide):
    step = cols
    while step > wide and step % 256 == 0:
        step //= 2
    return 16, step


def kernel(n, *refs):
    terms, weights, old_m, old_v = (refs[i : i + 3] for i in (0, 3, 6, 9))
    whole, new_m, new_v = (refs[i : i + 3] for i in (12, 15, 18))
    most, rest = refs[21:23], refs[23:25]
    slots, own, held = (refs[i : i + 3] for i in (25, 28, 31))
    sum_send, sum_recv, out_send, out_recv, own_sem, held_sem, m_sem, v_sem, rest_send, rest_recv, here, free = refs[34:]
    me = lax.axis_index("dp")
    right, left = lax.rem(me + 1, n), lax.rem(me + n - 1, n)
    ahead, behind, way = (right, left), (left, right), (1, -1)
    order = (2, 0, 1)
    units = [(w, d) for w in order for d in range(2)]
    rows = [m.shape[1] for m in new_m]

    def index(d, hops):
        return lax.rem(me - way[d] * hops + 2 * n, n)

    def block(w, owner):
        return pl.ds(pl.multiple_of(owner * rows[w], rows[w]), rows[w])

    def load_own(w, d, hops):
        return pltpu.make_async_copy(terms[w].at[0, d, block(w, index(d, hops))], own[w].at[d], own_sem.at[w, d])

    def load_held(w, d):
        return pltpu.make_async_copy(weights[w].at[d, block(w, me)], held[w].at[d], held_sem.at[w, d])

    def load_m(w, d):
        return pltpu.make_async_copy(old_m[w].at[d], new_m[w].at[d], m_sem.at[w, d])

    def load_v(w, d):
        return pltpu.make_async_copy(old_v[w].at[d], new_v[w].at[d], v_sem.at[w, d])

    def pass_sum(w, d, step, source):
        slot = lax.rem(step, SLOTS)
        return pltpu.make_async_remote_copy(
            src_ref=source,
            dst_ref=slots[w].at[d, slot],
            send_sem=sum_send.at[w, d],
            recv_sem=sum_recv.at[w, d, slot],
            device_id={"dp": ahead[d]},
            device_id_type=MESH,
        )

    def pass_new(w, d, step):
        piece = whole[w].at[d, block(w, index(d, step))]
        lands = piece
        if isinstance(step, int) and step == n - 3 and w < 2:
            first, count = (0, rows[0]) if w == 0 else (rows[0], rows[1] - TAIL)
            piece = whole[w].at[d, pl.ds(pl.multiple_of(index(d, step) * rows[w], rows[w]), count)]
            lands = most[d].at[pl.ds(first, count)]
        return pltpu.make_async_remote_copy(
            src_ref=piece,
            dst_ref=lands,
            send_sem=out_send.at[w, d],
            recv_sem=out_recv.at[w, d, step],
            device_id={"dp": ahead[d]},
            device_id_type=MESH,
        )

    def pass_rest(d):
        first = pl.multiple_of(index(d, n - 3) * rows[1] + (rows[1] - TAIL), 16)
        return pltpu.make_async_remote_copy(
            src_ref=whole[1].at[d, pl.ds(first, TAIL)],
            dst_ref=rest[d],
            send_sem=rest_send.at[d],
            recv_sem=rest_recv.at[d],
            device_id={"dp": ahead[d]},
            device_id_type=MESH,
        )

    def slot_of(w, d, step):
        return slots[w].at[d, lax.rem(step, SLOTS)]

    def over(w, wide, body):
        high, across = tiles(rows[w], whole[w].shape[2], wide)

        @pl.loop(0, rows[w] // high)
        def _(i):
            for c in range(0, whole[w].shape[2], across):
                body(pl.ds(pl.multiple_of(i * high, high), high), pl.ds(c, across))

    barrier = pltpu.get_barrier_semaphore()
    pl.semaphore_signal(barrier, inc=1, device_id={"dp": left}, device_id_type=MESH)
    pl.semaphore_wait(barrier, 1)
    pl.semaphore_signal(here, inc=1, device_id={"dp": right}, device_id_type=MESH)

    late = lax.rem(lax.axis_index("rep"), 2) == 0

    def load_rest():
        for w, d in units:
            load_held(w, d).start()
            load_m(w, d).start()
        for w, d in units:
            load_own(w, d, 2).start()
            load_v(w, d).start()

    @pl.when(late)
    def _():
        load_rest()
        for w, d in units:
            load_held(w, d).wait()
            load_m(w, d).wait()
            load_v(w, d).wait()

    def send_first(d):
        for w in order:
            pass_sum(w, d, 0, terms[w].at[0, d, block(w, index(d, 1))]).start()

    send_first(0)
    pl.when(jnp.logical_not(late))(load_rest)
    pl.semaphore_wait(here, 1)
    send_first(1)

    @pl.loop(1, n - 1)
    def _(step):
        for w in order:
            for d in range(2):
                pass_sum(w, d, step - 1, slot_of(w, d, step - 1)).wait_recv()
                pass_sum(w, d, step - 1, slot_of(w, d, step - 1)).wait_send()
                load_own(w, d, 0).wait()

                @pl.when((step >= 2) & (step < n - 2))
                def _():
                    pl.semaphore_signal(free.at[w, d], inc=1, device_id={"dp": behind[d]}, device_id_type=MESH)

            for d in range(2):
                so_far = slot_of(w, d, step - 1)

                def add(r, c, so_far=so_far, d=d):
                    so_far[r, c] = (so_far[r, c].astype(F32) + own[w][d, r, c].astype(F32)).astype(BF16)

                over(w, 1280, add)
            for d in range(2):
                load_own(w, d, step + 2).start()

                @pl.when(step >= SLOTS)
                def _():
                    pl.semaphore_wait(free.at[w, d], 1)

            for d in range(2):
                pass_sum(w, d, step, slot_of(w, d, step - 1)).start()

    for w in order:
        for d in range(2):
            pass_sum(w, d, n - 2, slot_of(w, d, n - 2)).wait_recv()
            pass_sum(w, d, n - 2, slot_of(w, d, n - 2)).wait_send()
            load_own(w, d, 0).wait()


            @pl.when(jnp.logical_not(late))
            def _():
                load_held(w, d).wait()
                load_m(w, d).wait()
                load_v(w, d).wait()

        for d in range(2):
            so_far = slot_of(w, d, n - 2)

            def adamw(r, c, so_far=so_far, d=d):
                g = (so_far[r, c].astype(F32) + own[w][d, r, c].astype(F32)).astype(BF16).astype(F32)
                m = 0.9 * new_m[w][d, r, c] + 0.1 * g
                v = 0.95 * new_v[w][d, r, c] + 0.05 * g * g
                step = m * lax.rsqrt(v + 1e-8) + 0.1 * held[w][d, r, c].astype(F32)
                new_m[w][d, r, c] = m
                new_v[w][d, r, c] = v
                mine = pl.multiple_of(me * rows[w], 16) + r.start
                whole[w][d, pl.ds(pl.multiple_of(mine, 16), 16), c] = (held[w][d, r, c].astype(F32) - 0.02 * step).astype(BF16)

            over(w, 640, adamw)
        for d in range(2):
            pass_new(w, d, 0).start()

    def forward(w, d, step):
        pass_new(w, d, step - 1).wait_recv()
        pass_new(w, d, step - 1).wait_send()
        pass_new(w, d, step).start()

    @pl.loop(1, n - 3)
    def _(step):
        for w, d in units:
            forward(w, d, step)

    for w, d in units:
        forward(w, d, n - 3)
        if w == 1:
            pass_rest(d).start()
    for w, d in units:
        if w == 2:
            forward(w, d, n - 2)
        else:
            pass_new(w, d, n - 3).wait()
    for d in range(2):
        pass_rest(d).wait()
        pass_new(2, d, n - 2).wait()


def put_out(n, *refs):
    arrays, most, rest, results = refs[:9], refs[9:11], refs[11:13], refs[13:22]
    sem, block_sem, rest_sem = refs[22:]
    me = lax.axis_index("dp")
    rows = arrays[0].shape[1] // n
    copies = []
    for i, (a, r) in enumerate(zip(arrays, results, strict=True)):
        for d in range(2):
            if i < 2:
                for hops in range(n - 1):
                    owner = lax.rem(me + (n - hops if d == 0 else hops), n)
                    piece = pl.ds(pl.multiple_of(owner * rows, rows), rows)
                    source = a.at[d, piece]
                    if hops == n - 2 and i == 0:
                        source = most[d].at[pl.ds(0, rows)]
                    elif hops == n - 2:
                        piece = pl.ds(pl.multiple_of(owner * rows, rows), rows - TAIL)
                        source = most[d].at[pl.ds(rows, rows - TAIL)]
                        tail = pl.ds(pl.multiple_of(owner * rows + (rows - TAIL), 16), TAIL)
                        copies.append(pltpu.make_async_copy(rest[d], r.at[d, tail], rest_sem.at[d]))
                    copies.append(pltpu.make_async_copy(source, r.at[d, piece], block_sem.at[i, d, hops]))
            else:
                copies.append(pltpu.make_async_copy(a.at[d], r.at[d], sem.at[i, d]))
    run(copies)


def run(copies):
    for one in copies:
        one.start()
    for one in copies:
        one.wait()


def put_most(n, gate, up, from_left, from_right, new_gate, new_up, sem):
    me = lax.axis_index("dp")
    rows = gate.shape[1] // n
    copies = []
    for d, one in enumerate((from_left, from_right)):
        owner = lax.rem(me + (1 if d == 0 else n - 1), n)
        for i, (result, first, count) in enumerate(((new_gate, 0, rows), (new_up, rows, rows - TAIL))):
            piece = pl.ds(pl.multiple_of(owner * rows, rows), count)
            copies.append(pltpu.make_async_copy(one.at[pl.ds(first, count)], result.at[d, piece], sem.at[i, d]))
    run(copies)


def put_rest(n, up, from_left, from_right, new_up, sem):
    me = lax.axis_index("dp")
    rows = up.shape[1] // n
    copies = []
    for d, one in enumerate((from_left, from_right)):
        owner = lax.rem(me + (1 if d == 0 else n - 1), n)
        piece = pl.ds(pl.multiple_of(owner * rows + (rows - TAIL), 16), TAIL)
        copies.append(pltpu.make_async_copy(one, new_up.at[d, piece], sem.at[d]))
    run(copies)


def solution(mesh):
    n = mesh.shape["dp"]

    def step(*arrays):
        terms, weights, m, v = (arrays[i : i + 3] for i in (0, 3, 6, 9))
        shard = [one.shape for one in m]
        cols = shard[0][2]
        hbm, vmem = pl.BlockSpec(memory_space=pltpu.HBM), pl.BlockSpec(memory_space=pltpu.VMEM)
        dma = pltpu.SemaphoreType.DMA
        inputs = (pltpu.with_memory_space_constraint(x, pltpu.HBM) for x in (*terms, *weights, *m, *v))
        made = pl.pallas_call(
            functools.partial(kernel, n),
            out_shape=(*(pltpu.VMEM(x.shape, x.dtype) for x in (*weights, *m, *v)), *(pltpu.VMEM((rows, cols), BF16) for rows in (2 * shard[0][1] - TAIL, TAIL) for _ in range(2))),
            in_specs=[hbm] * 12,
            out_specs=(vmem,) * 13,
            scratch_shapes=[
                *(pltpu.VMEM((2, SLOTS, *s[1:]), BF16) for s in shard),
                *(pltpu.VMEM(s, BF16) for s in shard),
                *(pltpu.VMEM(s, BF16) for s in shard),
                dma((3, 2)),
                dma((3, 2, SLOTS)),
                dma((3, 2)),
                dma((3, 2, n - 1)),
                dma((3, 2)),
                dma((3, 2)),
                dma((3, 2)),
                dma((3, 2)),
                dma((2,)),
                dma((2,)),
                pltpu.SemaphoreType.REGULAR,
                pltpu.SemaphoreType.REGULAR((3, 2)),
            ],
            compiler_params=pltpu.CompilerParams(collective_id=0, has_side_effects=True, vmem_limit_bytes=ROOM),
            name="step",
        )(*inputs)
        rings = [[(i, (i + way) % n) for i in range(n)] for way in (1, -1)]
        most, rest = ([lax.ppermute(made[at + d], "dp", rings[d]) for d in range(2)] for at in (9, 11))
        out = pl.pallas_call(
            functools.partial(put_out, n),
            out_shape=tuple(jax.ShapeDtypeStruct(x.shape, x.dtype) for x in (*weights, *m, *v)),
            in_specs=[vmem] * 13,
            out_specs=(hbm,) * 9,
            scratch_shapes=[dma((9, 2)), dma((2, 2, n - 1)), dma((2,))],
            compiler_params=pltpu.CompilerParams(has_side_effects=True, vmem_limit_bytes=ROOM),
            cost_estimate=pl.CostEstimate(flops=COST, bytes_accessed=80_000_000, transcendentals=0),
            name="put_out",
        )(*(pltpu.with_memory_space_constraint(x, pltpu.VMEM) for x in made))
        in_hbm, in_vmem = (functools.partial(pltpu.with_memory_space_constraint, memory_space=x) for x in (pltpu.HBM, pltpu.VMEM))
        gate, up = pl.pallas_call(
            functools.partial(put_most, n),
            out_shape=tuple(jax.ShapeDtypeStruct(x.shape, BF16) for x in weights[:2]),
            in_specs=[hbm, hbm, vmem, vmem],
            out_specs=(hbm, hbm),
            input_output_aliases={0: 0, 1: 1},
            scratch_shapes=[dma((2, 2))],
            compiler_params=pltpu.CompilerParams(has_side_effects=True, vmem_limit_bytes=ROOM),
            name="put_most",
        )(*map(in_hbm, out[:2]), *map(in_vmem, most))
        up = pl.pallas_call(
            functools.partial(put_rest, n),
            out_shape=jax.ShapeDtypeStruct(weights[1].shape, BF16),
            in_specs=[hbm, vmem, vmem],
            out_specs=hbm,
            input_output_aliases={0: 0},
            scratch_shapes=[dma((2,))],
            compiler_params=pltpu.CompilerParams(has_side_effects=True, vmem_limit_bytes=ROOM),
            name="put_rest",
        )(in_hbm(up), *map(in_vmem, rest))
        return (gate, up, *out[2:])

    all_of, cut = P(None, None, None), P(None, "dp", None)
    return jax.shard_map(
        step,
        mesh=mesh,
        in_specs=(P(("rep", "dp"), None, None, None),) * 3 + (all_of,) * 3 + (cut,) * 6,
        out_specs=(P("rep", None, None),) * 3 + (P("rep", "dp", None),) * 6,
        check_vma=False,
    )
```

```python
import functools

import jax
import jax.numpy as jnp
from jax import lax
from jax.experimental import pallas as pl
from jax.experimental.pallas import tpu as pltpu
from jax.sharding import PartitionSpec as P

MESH = pl.DeviceIdType.MESH
SLOTS = 3
TAIL = 32
COST = 100_000_000
ROOM = 17 * 2**20
F32, BF16 = jnp.float32, jnp.bfloat16


def tiles(rows, cols, wide):
    step = cols
    while step > wide and step % 256 == 0:
        step //= 2
    return 16, step


def kernel(n, *refs):
    terms, weights, old_m, old_v = (refs[i : i + 3] for i in (0, 3, 6, 9))
    whole, new_m, new_v = (refs[i : i + 3] for i in (12, 15, 18))
    most, rest = refs[21:23], refs[23:25]
    slots, own, held = (refs[i : i + 3] for i in (25, 28, 31))
    sum_send, sum_recv, out_send, out_recv, own_sem, held_sem, m_sem, v_sem, rest_send, rest_recv, free = refs[34:]
    me = lax.axis_index("dp")
    right, left = lax.rem(me + 1, n), lax.rem(me + n - 1, n)
    ahead, behind, way = (right, left), (left, right), (1, -1)
    order = (2, 0, 1)
    units = [(w, d) for w in order for d in range(2)]
    rows = [m.shape[1] for m in new_m]

    def index(d, hops):
        return lax.rem(me - way[d] * hops + 2 * n, n)

    def block(w, owner):
        return pl.ds(pl.multiple_of(owner * rows[w], rows[w]), rows[w])

    def load_own(w, d, hops):
        return pltpu.make_async_copy(terms[w].at[0, d, block(w, index(d, hops))], own[w].at[d], own_sem.at[w, d])

    def load_held(w, d):
        return pltpu.make_async_copy(weights[w].at[d, block(w, me)], held[w].at[d], held_sem.at[w, d])

    def load_m(w, d):
        return pltpu.make_async_copy(old_m[w].at[d], new_m[w].at[d], m_sem.at[w, d])

    def load_v(w, d):
        return pltpu.make_async_copy(old_v[w].at[d], new_v[w].at[d], v_sem.at[w, d])

    def pass_sum(w, d, step, source):
        slot = lax.rem(step, SLOTS)
        return pltpu.make_async_remote_copy(
            src_ref=source,
            dst_ref=slots[w].at[d, slot],
            send_sem=sum_send.at[w, d],
            recv_sem=sum_recv.at[w, d, slot],
            device_id={"dp": ahead[d]},
            device_id_type=MESH,
        )

    def pass_new(w, d, step):
        piece = whole[w].at[d, block(w, index(d, step))]
        lands = piece
        if isinstance(step, int) and step == n - 3 and w < 2:
            first, count = (0, rows[0]) if w == 0 else (rows[0], rows[1] - TAIL)
            piece = whole[w].at[d, pl.ds(pl.multiple_of(index(d, step) * rows[w], rows[w]), count)]
            lands = most[d].at[pl.ds(first, count)]
        return pltpu.make_async_remote_copy(
            src_ref=piece,
            dst_ref=lands,
            send_sem=out_send.at[w, d],
            recv_sem=out_recv.at[w, d, step],
            device_id={"dp": ahead[d]},
            device_id_type=MESH,
        )

    def pass_rest(d):
        first = pl.multiple_of(index(d, n - 3) * rows[1] + (rows[1] - TAIL), 16)
        return pltpu.make_async_remote_copy(
            src_ref=whole[1].at[d, pl.ds(first, TAIL)],
            dst_ref=rest[d],
            send_sem=rest_send.at[d],
            recv_sem=rest_recv.at[d],
            device_id={"dp": ahead[d]},
            device_id_type=MESH,
        )

    def slot_of(w, d, step):
        return slots[w].at[d, lax.rem(step, SLOTS)]

    def over(w, wide, body):
        high, across = tiles(rows[w], whole[w].shape[2], wide)

        @pl.loop(0, rows[w] // high)
        def _(i):
            for c in range(0, whole[w].shape[2], across):
                body(pl.ds(pl.multiple_of(i * high, high), high), pl.ds(c, across))

    barrier = pltpu.get_barrier_semaphore()
    for other in (left, right):
        pl.semaphore_signal(barrier, inc=1, device_id={"dp": other}, device_id_type=MESH)
    pl.semaphore_wait(barrier, 2)

    late = lax.rem(lax.axis_index("rep"), 2) == 0

    def load_state(w, d):
        load_held(w, d).start()
        load_m(w, d).start()
        load_v(w, d).start()

    @pl.when(late)
    def _():
        for w, d in units:
            load_state(w, d)
        for w, d in units:
            load_held(w, d).wait()
            load_m(w, d).wait()

    for w, d in units:
        pass_sum(w, d, 0, terms[w].at[0, d, block(w, index(d, 1))]).start()
    for w, d in units:
        load_own(w, d, 2).start()

    @pl.loop(1, n - 1)
    def _(step):
        for w in order:
            for d in range(2):
                pass_sum(w, d, step - 1, slot_of(w, d, step - 1)).wait_recv()
                pass_sum(w, d, step - 1, slot_of(w, d, step - 1)).wait_send()
                load_own(w, d, 0).wait()

                @pl.when((step >= 2) & (step < n - 2))
                def _():
                    pl.semaphore_signal(free.at[w, d], inc=1, device_id={"dp": behind[d]}, device_id_type=MESH)

            for d in range(2):
                so_far = slot_of(w, d, step - 1)

                def add(r, c, so_far=so_far, d=d):
                    so_far[r, c] = (so_far[r, c].astype(F32) + own[w][d, r, c].astype(F32)).astype(BF16)

                over(w, 1280, add)
            for d in range(2):
                load_own(w, d, step + 2).start()
                pl.when((step == 1) & jnp.logical_not(late))(functools.partial(load_state, w, d))

                @pl.when(step >= SLOTS)
                def _():
                    pl.semaphore_wait(free.at[w, d], 1)

            for d in range(2):
                pass_sum(w, d, step, slot_of(w, d, step - 1)).start()

    for w in order:
        for d in range(2):
            pass_sum(w, d, n - 2, slot_of(w, d, n - 2)).wait_recv()
            pass_sum(w, d, n - 2, slot_of(w, d, n - 2)).wait_send()
            load_own(w, d, 0).wait()

            load_v(w, d).wait()

            @pl.when(jnp.logical_not(late))
            def _():
                load_held(w, d).wait()
                load_m(w, d).wait()

        for d in range(2):
            so_far = slot_of(w, d, n - 2)

            def adamw(r, c, so_far=so_far, d=d):
                g = (so_far[r, c].astype(F32) + own[w][d, r, c].astype(F32)).astype(BF16).astype(F32)
                m = 0.9 * new_m[w][d, r, c] + 0.1 * g
                v = 0.95 * new_v[w][d, r, c] + 0.05 * g * g
                step = m * lax.rsqrt(v + 1e-8) + 0.1 * held[w][d, r, c].astype(F32)
                new_m[w][d, r, c] = m
                new_v[w][d, r, c] = v
                mine = pl.multiple_of(me * rows[w], 16) + r.start
                whole[w][d, pl.ds(pl.multiple_of(mine, 16), 16), c] = (held[w][d, r, c].astype(F32) - 0.02 * step).astype(BF16)

            over(w, 640, adamw)
        for d in range(2):
            pass_new(w, d, 0).start()

    def forward(w, d, step):
        pass_new(w, d, step - 1).wait_recv()
        pass_new(w, d, step - 1).wait_send()
        pass_new(w, d, step).start()

    @pl.loop(1, n - 3)
    def _(step):
        for w, d in units:
            forward(w, d, step)

    for w, d in units:
        forward(w, d, n - 3)
        if w == 1:
            pass_rest(d).start()
    for w, d in units:
        if w == 2:
            forward(w, d, n - 2)
        else:
            pass_new(w, d, n - 3).wait()
    for d in range(2):
        pass_rest(d).wait()
        pass_new(2, d, n - 2).wait()


def put_out(n, *refs):
    arrays, most, rest, results = refs[:9], refs[9:11], refs[11:13], refs[13:22]
    sem, block_sem, rest_sem = refs[22:]
    me = lax.axis_index("dp")
    rows = arrays[0].shape[1] // n
    copies = []
    for i, (a, r) in enumerate(zip(arrays, results, strict=True)):
        for d in range(2):
            if i < 2:
                for hops in range(n - 1):
                    owner = lax.rem(me + (n - hops if d == 0 else hops), n)
                    piece = pl.ds(pl.multiple_of(owner * rows, rows), rows)
                    source = a.at[d, piece]
                    if hops == n - 2 and i == 0:
                        source = most[d].at[pl.ds(0, rows)]
                    elif hops == n - 2:
                        piece = pl.ds(pl.multiple_of(owner * rows, rows), rows - TAIL)
                        source = most[d].at[pl.ds(rows, rows - TAIL)]
                        tail = pl.ds(pl.multiple_of(owner * rows + (rows - TAIL), 16), TAIL)
                        copies.append(pltpu.make_async_copy(rest[d], r.at[d, tail], rest_sem.at[d]))
                    copies.append(pltpu.make_async_copy(source, r.at[d, piece], block_sem.at[i, d, hops]))
            else:
                copies.append(pltpu.make_async_copy(a.at[d], r.at[d], sem.at[i, d]))
    run(copies)


def run(copies):
    for one in copies:
        one.start()
    for one in copies:
        one.wait()


def put_most(n, gate, up, from_left, from_right, new_gate, new_up, sem):
    me = lax.axis_index("dp")
    rows = gate.shape[1] // n
    copies = []
    for d, one in enumerate((from_left, from_right)):
        owner = lax.rem(me + (1 if d == 0 else n - 1), n)
        for i, (result, first, count) in enumerate(((new_gate, 0, rows), (new_up, rows, rows - TAIL))):
            piece = pl.ds(pl.multiple_of(owner * rows, rows), count)
            copies.append(pltpu.make_async_copy(one.at[pl.ds(first, count)], result.at[d, piece], sem.at[i, d]))
    run(copies)


def put_rest(n, up, from_left, from_right, new_up, sem):
    me = lax.axis_index("dp")
    rows = up.shape[1] // n
    copies = []
    for d, one in enumerate((from_left, from_right)):
        owner = lax.rem(me + (1 if d == 0 else n - 1), n)
        piece = pl.ds(pl.multiple_of(owner * rows + (rows - TAIL), 16), TAIL)
        copies.append(pltpu.make_async_copy(one, new_up.at[d, piece], sem.at[d]))
    run(copies)


def solution(mesh):
    n = mesh.shape["dp"]

    def step(*arrays):
        terms, weights, m, v = (arrays[i : i + 3] for i in (0, 3, 6, 9))
        shard = [one.shape for one in m]
        cols = shard[0][2]
        hbm, vmem = pl.BlockSpec(memory_space=pltpu.HBM), pl.BlockSpec(memory_space=pltpu.VMEM)
        dma = pltpu.SemaphoreType.DMA
        inputs = (pltpu.with_memory_space_constraint(x, pltpu.HBM) for x in (*terms, *weights, *m, *v))
        made = pl.pallas_call(
            functools.partial(kernel, n),
            out_shape=(*(pltpu.VMEM(x.shape, x.dtype) for x in (*weights, *m, *v)), *(pltpu.VMEM((rows, cols), BF16) for rows in (2 * shard[0][1] - TAIL, TAIL) for _ in range(2))),
            in_specs=[hbm] * 12,
            out_specs=(vmem,) * 13,
            scratch_shapes=[
                *(pltpu.VMEM((2, SLOTS, *s[1:]), BF16) for s in shard),
                *(pltpu.VMEM(s, BF16) for s in shard),
                *(pltpu.VMEM(s, BF16) for s in shard),
                dma((3, 2)),
                dma((3, 2, SLOTS)),
                dma((3, 2)),
                dma((3, 2, n - 1)),
                dma((3, 2)),
                dma((3, 2)),
                dma((3, 2)),
                dma((3, 2)),
                dma((2,)),
                dma((2,)),
                pltpu.SemaphoreType.REGULAR((3, 2)),
            ],
            compiler_params=pltpu.CompilerParams(collective_id=0, has_side_effects=True, vmem_limit_bytes=ROOM),
            name="step",
        )(*inputs)
        rings = [[(i, (i + way) % n) for i in range(n)] for way in (1, -1)]
        most, rest = ([lax.ppermute(made[at + d], "dp", rings[d]) for d in range(2)] for at in (9, 11))
        out = pl.pallas_call(
            functools.partial(put_out, n),
            out_shape=tuple(jax.ShapeDtypeStruct(x.shape, x.dtype) for x in (*weights, *m, *v)),
            in_specs=[vmem] * 13,
            out_specs=(hbm,) * 9,
            scratch_shapes=[dma((9, 2)), dma((2, 2, n - 1)), dma((2,))],
            compiler_params=pltpu.CompilerParams(has_side_effects=True, vmem_limit_bytes=ROOM),
            cost_estimate=pl.CostEstimate(flops=COST, bytes_accessed=80_000_000, transcendentals=0),
            name="put_out",
        )(*(pltpu.with_memory_space_constraint(x, pltpu.VMEM) for x in made))
        in_hbm, in_vmem = (functools.partial(pltpu.with_memory_space_constraint, memory_space=x) for x in (pltpu.HBM, pltpu.VMEM))
        gate, up = pl.pallas_call(
            functools.partial(put_most, n),
            out_shape=tuple(jax.ShapeDtypeStruct(x.shape, BF16) for x in weights[:2]),
            in_specs=[hbm, hbm, vmem, vmem],
            out_specs=(hbm, hbm),
            input_output_aliases={0: 0, 1: 1},
            scratch_shapes=[dma((2, 2))],
            compiler_params=pltpu.CompilerParams(has_side_effects=True, vmem_limit_bytes=ROOM),
            name="put_most",
        )(*map(in_hbm, out[:2]), *map(in_vmem, most))
        up = pl.pallas_call(
            functools.partial(put_rest, n),
            out_shape=jax.ShapeDtypeStruct(weights[1].shape, BF16),
            in_specs=[hbm, vmem, vmem],
            out_specs=hbm,
            input_output_aliases={0: 0},
            scratch_shapes=[dma((2,))],
            compiler_params=pltpu.CompilerParams(has_side_effects=True, vmem_limit_bytes=ROOM),
            name="put_rest",
        )(in_hbm(up), *map(in_vmem, rest))
        return (gate, up, *out[2:])

    all_of, cut = P(None, None, None), P(None, "dp", None)
    return jax.shard_map(
        step,
        mesh=mesh,
        in_specs=(P(("rep", "dp"), None, None, None),) * 3 + (all_of,) * 3 + (cut,) * 6,
        out_specs=(P("rep", None, None),) * 3 + (P("rep", "dp", None),) * 6,
        check_vma=False,
    )
```
